32 devices in a mesh: dp: 4 (over y, core), tensor: 8 (over z, x).
Axes of the slice: x: 2, y: 2, z: 4, core: 2. Of those that a mesh axis runs over, the one named last changes fastest.
Arguments:
- tokens: bfloat16 [512, 1024], P('dp', 'tensor'), may hold values from -6 to 6
- init_noise: float32 [512, 1024], P('dp', 'tensor'), may hold values from -1 to 1
- segment_ids: int32 [512], P('dp'), may hold values from 0 to 7, never falling along the last dimension, each value on 1 to 256 neighbouring positions
- target: float32 [512, 1024], P('dp', 'tensor'), may hold values from -6 to 6
- norm_gain: float32 [1024], replicated, may hold values from 0.1 to 1.9
- weight_in: bfloat16 [1024, 32768], P(None, 'tensor'), may hold values from -0.1875 to 0.1875
- weight_out: bfloat16 [32768, 1024], P('tensor'), may hold values from -0.03125 to 0.03125
- moment_in: float32 [1024, 32768], P('dp', 'tensor'), may hold values from -1.5 to 1.5
- moment_out: float32 [32768, 1024], P('tensor', 'dp'), may hold values from -1.5 to 1.5
Outputs:
- new_weight_in: bfloat16 [1024, 32768], P('dp', 'tensor')
- new_weight_out: bfloat16 [32768, 1024], P('tensor', 'dp')
- new_moment_in: float32 [1024, 32768], P('dp', 'tensor')
- new_moment_out: float32 [32768, 1024], P('tensor', 'dp')
- perturbation: float32 [512, 1024], P('dp', 'tensor')
The draws below stay inside these ranges and needn't reach their ends.
Inputs may be any that keep to these rules, and one draw needn't show every extreme that they name: `segment_ids`: example ids never fall along the tokens; every example holds 1 to 256 tokens.
All inputs are finite; a program needn't handle non-finite values.
Results may differ from the reference program's by a relative error of at most 0.0051.
Values may be sent and summed in bfloat16 or wider, within the bound.
A program may use at most 128 MiB of HBM per device.

```python
import math
import jax
import jax.numpy as jnp
import numpy as np
from jax import lax

D = 1024
FF = 32768
ASCENTS = 2
TOKENS = 512
EXAMPLES = 8
MOST = 256
N_TENSOR = 8


def shard_levels(key, shape, cuts, least, high):
    def one(axis_at, blocks):
        steps = jax.random.uniform(jax.random.fold_in(jax.random.fold_in(key, 6), axis_at), (blocks,), jnp.float32, least / len(cuts), high / len(cuts))
        return jnp.repeat(jnp.exp(steps), shape[axis_at] // blocks).reshape((-1,) + (1,) * (len(shape) - axis_at - 1))

    gain = one(*cuts[0])
    for cut in cuts[1:]:
        gain = gain * one(*cut)
    return gain


def length_profile(number_of, total, limit, skew):
    weights = [(1 << 20) // math.isqrt(grade ** skew) + 1 for grade in range(2, number_of + 1)]
    surplus, given = total - limit - (number_of - 1), [1] * (number_of - 1)
    while surplus > 0:
        movable = [i for i in range(number_of - 1) if given[i] < limit]
        whole, remaining = sum([weights[i] for i in movable]), surplus
        for i in movable:
            more = min(limit - given[i], max(1, remaining * weights[i] // whole), surplus)
            given[i] = given[i] + more
            surplus = surplus - more
    return np.array([limit] + given)


def uneven(own_key, count, total, most, slope):
    if count == 2:
        one = jax.random.randint(own_key, (), max(1, total - most), min(most, total - 1) + 1)
        return jnp.stack([one, total - one])
    sizes = jnp.asarray(length_profile(count, total, most, slope), jnp.int32)
    couples = (count - 1) // 2
    giver, taker = sizes[1:1 + 2 * couples:2], sizes[2:2 + 2 * couples:2]
    room = jnp.minimum(giver - 1, most - taker)
    shifted = jax.random.randint(jax.random.fold_in(own_key, 1), (couples,), 0, 1 << 20) % (room + 1)
    sizes = sizes.at[1:1 + 2 * couples:2].set(giver - shifted).at[2:2 + 2 * couples:2].set(taker + shifted)
    return sizes[jax.random.permutation(jax.random.fold_in(own_key, 2), count)]


def scatter_about(stream_key, shape, width, most, pieces=(), held_as=jnp.bfloat16):
    gain = shard_levels(stream_key, shape, pieces, -0.22, 0.18) if pieces else 1.0
    result = jax.random.normal(stream_key, shape, jnp.float32) * width * gain
    return jnp.minimum(jnp.maximum(result, -most), most).astype(held_as)


def setup_inputs(seed: int = 0) -> dict:
    seeds = jax.random.split(jax.random.key(seed), 10)
    return {
        "tokens": scatter_about(seeds[0], (TOKENS, D), 1.0, 6.0, ((0, 4), (1, 8))),
        "init_noise": jnp.clip(jax.random.uniform(seeds[1], (TOKENS, D), jnp.float32, -1.0, 1.0) * shard_levels(seeds[1], (TOKENS, D), ((0, 4), (1, 8)), -0.4, 0.0), -1.0, 1.0),
        "segment_ids": jnp.searchsorted(jnp.cumsum(uneven(seeds[2], EXAMPLES, TOKENS, MOST, 1)), jnp.arange(TOKENS), side="right").astype(jnp.int32),
        "target": scatter_about(seeds[3], (TOKENS, D), 1.0, 6.0, ((0, 4), (1, 8)), jnp.float32),
        "norm_gain": jnp.clip(1.0 + 0.18 * jax.random.normal(seeds[4], (D,), jnp.float32), 0.1, 1.9),
        "weight_in": scatter_about(seeds[5], (D, FF), D ** -0.5, 0.1875, ((1, 8),)),
        "weight_out": scatter_about(seeds[6], (FF, D), FF ** -0.5, 0.03125, ((0, 8),)),
        "moment_in": scatter_about(seeds[7], (D, FF), 0.1, 1.5, ((0, 4), (1, 8)), jnp.float32),
        "moment_out": scatter_about(seeds[8], (FF, D), 0.1, 1.5, ((0, 8), (1, 4)), jnp.float32),
    }


coeff = 0.7978845608
adv_init = 0.5
adv_step = 0.5
decay = 0.9
learn_rate = 0.01

def gelu_value(values):
    tangent = jnp.tanh(coeff * (values + 0.044715 * values * values * values))
    return 0.5 * values * (1.0 + tangent)

def gelu_slope(values):
    tangent = jnp.tanh(coeff * (values + 0.044715 * values * values * values))
    return 0.5 * (1.0 + tangent) + 0.5 * values * (1.0 - tangent * tangent) * coeff * (1.0 + 3.0 * 0.044715 * values * values)

def reference(tokens, init_noise, segment_ids, target, norm_gain, weight_in, weight_out, moment_in, moment_out):
    block = FF // N_TENSOR
    loss_scale = 1.0 / math.sqrt(TOKENS)
    weights_in = weight_in.reshape(D, N_TENSOR, block).transpose(1, 0, 2)
    weights_out = weight_out.reshape(N_TENSOR, block, D)
    labels = jnp.arange(EXAMPLES, dtype=jnp.int32)
    onehot = (segment_ids[:, None] == labels[None, :]).astype(jnp.float32)
    counts = lax.optimization_barrier(jnp.sum(onehot, axis=0))
    perturb = adv_init * init_noise
    grads_in = jnp.zeros((D, FF), jnp.float32)
    grads_out = jnp.zeros((FF, D), jnp.float32)
    for ascent in range(ASCENTS):
        embedded = tokens.astype(jnp.float32) + perturb
        emb_bf = lax.optimization_barrier(embedded.astype(jnp.bfloat16))
        emb_float = emb_bf.astype(jnp.float32)
        inv_rms = lax.rsqrt(lax.optimization_barrier(jnp.mean(emb_float * emb_float, axis=1, keepdims=True)) + 1e-06)
        normed = (emb_float * inv_rms * norm_gain).astype(jnp.bfloat16)

        def forward(running, weights):
            preact = jnp.dot(normed, weights[0], preferred_element_type=jnp.float32)
            hidden = gelu_value(preact).astype(jnp.bfloat16)
            return (running + jnp.dot(hidden, weights[1], preferred_element_type=jnp.float32), None)
        mixed, _ = lax.scan(forward, jnp.zeros((TOKENS, D), jnp.float32), (weights_in, weights_out))
        out_grad = (embedded + mixed - target) * loss_scale
        grad_bf = out_grad.astype(jnp.bfloat16)

        def backward(running, weights):
            preact = jnp.dot(normed, weights[0], preferred_element_type=jnp.float32)
            hidden = gelu_value(preact).astype(jnp.bfloat16)
            hidden_grad = (jnp.dot(grad_bf, weights[1].T, preferred_element_type=jnp.float32) * gelu_slope(preact)).astype(jnp.bfloat16)
            part_in = jnp.dot(normed.T, hidden_grad, preferred_element_type=jnp.float32)
            part_out = jnp.dot(hidden.T, grad_bf, preferred_element_type=jnp.float32)
            running = running + jnp.dot(hidden_grad, weights[0].T, preferred_element_type=jnp.float32)
            return (running, (part_in, part_out))
        normed_grad, (parts_in, parts_out) = lax.scan(backward, jnp.zeros((TOKENS, D), jnp.float32), (weights_in, weights_out))
        grads_in = grads_in + parts_in.transpose(1, 0, 2).reshape(D, FF)
        grads_out = grads_out + parts_out.reshape(FF, D)
        if ascent + 1 < ASCENTS:
            scaled = normed_grad * norm_gain
            row_dot = lax.optimization_barrier(jnp.sum(scaled * emb_float, axis=1, keepdims=True))
            delta_grad = out_grad + inv_rms * scaled - emb_float * inv_rms * inv_rms * inv_rms * row_dot / D
            row_squares = lax.optimization_barrier(jnp.sum(delta_grad * delta_grad, axis=1))
            square_sums = lax.optimization_barrier(jnp.sum(onehot * row_squares[:, None], axis=0))
            root_mean = jnp.sqrt(square_sums / (counts * D) + 1e-06)
            token_scale = lax.optimization_barrier(jnp.sum(onehot * (adv_step / root_mean)[None, :], axis=1))
            perturb = perturb + delta_grad * token_scale[:, None]
    new_moment_in = decay * moment_in + grads_in / ASCENTS
    new_moment_out = decay * moment_out + grads_out / ASCENTS
    new_weight_in = (weight_in.astype(jnp.float32) - learn_rate * new_moment_in).astype(jnp.bfloat16)
    new_weight_out = (weight_out.astype(jnp.float32) - learn_rate * new_moment_out).astype(jnp.bfloat16)
    return (new_weight_in, new_weight_out, new_moment_in, new_moment_out, perturb)
```

```python
import functools

import jax
import jax.numpy as jnp
from jax import lax
from jax.experimental import pallas as pl
from jax.experimental.pallas import tpu as pltpu
from jax.sharding import PartitionSpec as P

ASCENTS = 2

coeff = 0.7978845608
cubic = 0.044715
adv_init = 0.5
adv_step = 0.5
decay = 0.9
learn_rate = 0.01
LANES = 128
CHUNK = 256
F32, BF16 = jnp.float32, jnp.bfloat16


def gelu_both(values):
    square = values * values
    half = 0.5 + 0.5 * jnp.tanh(values * (coeff + (coeff * cubic) * square))
    hidden = values * half
    slope = half + (hidden * (1.0 - half)) * (2.0 * coeff + (6.0 * coeff * cubic) * square)
    return hidden, slope


def dot_nt(left, right):
    return lax.dot_general(left, right, (((1,), (1,)), ((), ())), preferred_element_type=F32)


def dot_nn(left, right):
    return jnp.dot(left, right, preferred_element_type=F32)


class Place:
    def __init__(self):
        self.dp_count, self.tensor_count = lax.axis_size("dp"), lax.axis_size("tensor")
        self.ys, self.zs = self.dp_count // 2, self.tensor_count // 2
        self.dp, self.tensor = lax.axis_index("dp"), lax.axis_index("tensor")
        self.y, self.core = self.dp // 2, self.dp % 2
        self.z, self.x = self.tensor // 2, self.tensor % 2


def enter(at):
    barrier = pltpu.get_barrier_semaphore()
    for step in range(1, at.tensor_count):
        there = (at.dp, lax.rem(at.tensor + step, at.tensor_count))
        pl.semaphore_signal(barrier, inc=1, device_id=there, device_id_type=pl.DeviceIdType.MESH)
    for step in range(1, at.dp_count):
        there = (lax.rem(at.dp + step, at.dp_count), at.tensor)
        pl.semaphore_signal(barrier, inc=1, device_id=there, device_id_type=pl.DeviceIdType.MESH)
    pl.semaphore_wait(barrier, at.tensor_count + at.dp_count - 2)


def send(source, target, sems, number, there):
    copy = pltpu.make_async_remote_copy(
        src_ref=source,
        dst_ref=target,
        send_sem=sems[0].at[number],
        recv_sem=sems[1].at[number],
        device_id=there,
        device_id_type=pl.DeviceIdType.MESH,
    )
    copy.start()
    return copy


def gather_copies(dp_count, tensor_count):
    return tensor_count - 1 + dp_count - 1


class Gather:
    def __init__(self, at, own_ref, whole_ref, sems):
        self.at, self.whole, self.sems = at, whole_ref, sems
        self.rows, self.cols = own_ref.shape
        self.numbers = iter(range(gather_copies(at.dp_count, at.tensor_count)))
        self.flat = len(whole_ref.shape) == 2
        self.started = []
        self.other_x = (at.dp, at.z * 2 + 1 - at.x)
        self.partner = (at.y * 2 + 1 - at.core, at.tensor)
        whole_ref[self.place(at.dp, at.tensor)] = own_ref[...]
        self.along_z = [
            self.start(
                own_ref, self.block(at.dp, at.tensor),
                (at.dp, lax.rem(at.z + at.zs - k, at.zs) * 2 + at.x),
            )
            for k in range(1, at.zs)
        ]
        self.along_x = [self.start(own_ref, self.block(at.dp, at.tensor), self.other_x)]

    def span(self, dp):
        return pl.ds(pl.multiple_of(dp * self.rows, self.rows), self.rows)

    def place(self, dp, tensor):
        if self.flat:
            return (self.span(dp), pl.ds(pl.multiple_of(tensor * self.cols, self.cols), self.cols))
        return (tensor, self.span(dp))

    def block(self, dp, tensor):
        return self.whole.at[self.place(dp, tensor)]

    def strip(self, dp):
        return self.whole.at[self.span(dp)] if self.flat else self.whole.at[:, self.span(dp)]

    def start(self, source, target, there):
        copy = send(source, target, self.sems, next(self.numbers), there)
        self.started.append(copy)
        return copy

    def spread(self):
        at = self.at
        for k in range(1, at.zs):
            self.along_z[k - 1].wait_recv()
            block = self.block(at.dp, lax.rem(at.z + k, at.zs) * 2 + at.x)
            self.along_x.append(self.start(block, block, self.other_x))

    def land(self):
        for copy in self.along_x:
            copy.wait_recv()

    def share(self):
        at, strip = self.at, self.strip(self.at.dp)
        self.along_y = {
            j: self.start(
                strip, strip, (lax.rem(at.y + at.ys - j, at.ys) * 2 + at.core, at.tensor)
            )
            for j in range(1, at.ys)
        }
        self.to_core = {0: self.start(strip, strip, self.partner)}

    def from_y(self, j):
        at = self.at
        self.along_y[j].wait_recv()
        strip = self.strip(lax.rem(at.y + j, at.ys) * 2 + at.core)
        self.to_core[j] = self.start(strip, strip, self.partner)

    def from_core(self, j):
        self.to_core[j].wait_recv()

    def done(self):
        for copy in self.started:
            copy.wait_send()

    def row_block(self, dp):
        if self.flat:
            return self.whole[self.span(dp), :]
        return jnp.concatenate(
            [self.whole[t, self.span(dp), :] for t in range(self.at.tensor_count)], axis=1
        )

    def columns_of(self, dp, column, width):
        if self.flat:
            return self.whole[self.span(dp), pl.ds(pl.multiple_of(column, width), width)]
        first = column // self.cols
        return jnp.concatenate(
            [self.whole[first + i, self.span(dp), :] for i in range(width // self.cols)], axis=1
        )


class ScatterSum:
    def __init__(self, at, outgoing, landing, kept, sems):
        self.at, self.outgoing, self.landing, self.kept, self.sems = (
            at, outgoing, landing, kept, sems
        )
        self.cols = outgoing.shape[2]
        self.group = CHUNK // self.cols
        self.chunks = at.tensor_count // self.group
        self.inner = at.tensor % self.group
        self.copies = {}

    def order(self):
        half = self.chunks // 2
        return sorted(range(self.chunks), key=lambda k: (k == 0, abs(k - half)))

    def chunk(self, k):
        return lax.rem(self.at.tensor // self.group + k, self.chunks)

    def give(self, k, value):
        first = self.chunk(k) * self.group
        for i in range(self.group):
            part = value[:, i * self.cols:(i + 1) * self.cols]
            self.outgoing[first + i] = part.astype(BF16)
            if k == 0:
                self.kept[i] = part
        for j in range(self.group):
            label = k * self.group + j
            if label:
                there = first + lax.rem(self.inner + j, self.group)
                self.copies[label] = send(
                    self.outgoing.at[there], self.landing.at[label - 1], self.sems, label - 1,
                    (self.at.dp, there),
                )

    def take(self):
        value = self.kept[self.inner]
        for label, copy in self.copies.items():
            copy.wait_recv()
            value = value + self.landing[label - 1].astype(F32)
        for copy in self.copies.values():
            copy.wait_send()
        return value


class SmallSum:
    def __init__(self, at, axis, out, landing, sems):
        count = at.dp_count if axis == "dp" else at.tensor_count
        self.out, self.landing, self.copies = out, landing, []
        for step in range(1, count):
            if axis == "dp":
                there = (lax.rem(at.dp + step, count), at.tensor)
            else:
                there = (at.dp, lax.rem(at.tensor + step, count))
            self.copies.append(send(out, landing.at[step - 1], sems, step - 1, there))

    def take(self):
        value = self.out[...]
        for step, copy in enumerate(self.copies):
            copy.wait_recv()
            value = value + self.landing[step]
        for copy in self.copies:
            copy.wait_send()
        return value


def own_part(value, offset, size, axis):
    parts = [lax.slice_in_dim(value, s, s + size, axis=axis) for s in range(0, value.shape[axis], size)]
    result = parts[0]
    for i, part in enumerate(parts[1:], 1):
        result = jnp.where(offset == i * size, part, result)
    return result


def step_kernel(
    tokens_ref, noise_ref, ids_ref, target_ref, gain_ref, win_hbm, wout_hbm, min_hbm, mout_hbm,
    hidden, hgrad, turn_in, turn_out, acc_in, acc_out, mom_in, mom_out, own_in, own_out, perturb_ref,
    win, wout, emb_all, grad_all, normed, grad_flat, own_emb, own_grad, out_grad_ref, inv_ref,
    onehot_ref, kept, outgoing, landing_1, landing_2, landing_3,
    table_out, table_in, square_out, square_in, square_out_dp, square_in_dp, count_out, count_in,
    load_sems, late_sems, *sems, scale, features,
):
    at = Place()
    rows, width = tokens_ref.shape
    hidden_units = win.shape[1]
    total = hidden.shape[0]
    own_cols = acc_in.shape[0]
    pairs = [(sems[2 * i], sems[2 * i + 1]) for i in range(len(sems) // 2)]
    gather_sems, sum_sems = pairs[:4], pairs[4:7]
    table_sems, square_sems, square_dp_sems, count_sems = pairs[7:11]
    narrow = len(emb_all.shape) == 3

    loads = [
        pltpu.make_async_copy(win_hbm, win, load_sems.at[0]),
        pltpu.make_async_copy(wout_hbm, wout, load_sems.at[1]),
    ]
    for load in loads:
        load.start()
    block_cols = own_out.shape[1]
    first_col = at.dp * own_cols // block_cols * block_cols
    late = [
        pltpu.make_async_copy(
            win_hbm.at[pl.ds(pl.multiple_of(at.dp * own_cols, own_cols), own_cols)], own_in,
            late_sems.at[0],
        ),
        pltpu.make_async_copy(
            wout_hbm.at[:, pl.ds(pl.multiple_of(first_col, block_cols), block_cols)], own_out,
            late_sems.at[1],
        ),
        pltpu.make_async_copy(min_hbm, mom_in, late_sems.at[2]),
        pltpu.make_async_copy(mout_hbm, mom_out, late_sems.at[3]),
    ]
    tokens = tokens_ref[...].astype(F32)
    own_emb[0] = (tokens + adv_init * noise_ref[...]).astype(BF16)
    enter(at)
    emb = Gather(at, own_emb.at[0], emb_all, gather_sems[0])

    lane = lax.broadcasted_iota(jnp.int32, (rows, rows), 1).astype(F32)
    ids = jnp.broadcast_to(ids_ref[...].astype(F32), (rows, rows)).T
    onehot = (ids == lane).astype(F32)
    onehot_ref[...] = onehot
    count_out[...] = jnp.broadcast_to(jnp.sum(onehot, axis=0, keepdims=True), (8, rows))
    counting = SmallSum(at, "dp", count_out, count_in, count_sems)
    group = max(width, LANES)
    first = at.tensor * width // group * group
    gain_own = own_part(
        gain_ref[:, pl.ds(pl.multiple_of(first, group), group)], at.tensor * width - first, width, 1
    )

    def span(dp):
        return pl.ds(pl.multiple_of(dp * rows, rows), rows)

    def norm(gather, dp, keep=False):
        block = gather.row_block(dp).astype(F32)
        inv = lax.rsqrt(jnp.mean(block * block, axis=1, keepdims=True) + 1e-06)
        normed[span(dp), :] = (block * inv * gain_ref[...]).astype(BF16)
        if keep:
            inv_ref[...] = jnp.broadcast_to(inv, inv_ref.shape)

    tile = 512

    def tiles(body, count=1):
        @pl.loop(0, hidden_units // tile)
        def _(i):
            body(pl.ds(pl.multiple_of(i * tile, tile), tile))

    def forward(dp):
        def body(cols):
            value, slope = gelu_both(dot_nn(normed[span(dp), :], win[:, cols]))
            hidden[span(dp), cols] = value.astype(BF16)
            hgrad[span(dp), cols] = slope.astype(BF16)

        tiles(body)

    def flat_grad(gather, dp):
        if narrow:
            grad_flat[span(dp), :] = gather.row_block(dp)

    grad_source = grad_flat if narrow else grad_all

    def backward(dp):
        def body(cols):
            value = dot_nt(grad_source[span(dp), :], wout[cols, :])
            hgrad[span(dp), cols] = (value * hgrad[span(dp), cols].astype(F32)).astype(BF16)

        tiles(body)

    def turned(source):
        block = max(own_cols, LANES)
        start = at.dp * own_cols // block * block
        value = source[:, pl.ds(pl.multiple_of(start, block), block)].astype(F32).T
        return own_part(value, at.dp * own_cols - start, own_cols, 0).astype(BF16)

    def weight_grads():
        def body(cols):
            acc_in[:, cols] = dot_nn(turn_in[...], hgrad[:, cols])

        tiles(body)

        def body(cols):
            acc_out[:, cols] = dot_nn(turn_out[...], hidden[:, cols])

        tiles(body)

    def partial_out(number, landing):
        sums = ScatterSum(at, outgoing, landing, kept, sum_sems[number])
        for k in sums.order():
            column = pl.multiple_of(sums.chunk(k) * CHUNK, CHUNK)
            sums.give(k, dot_nn(hidden[span(at.dp), :], wout[:, pl.ds(column, CHUNK)]))
        return sums

    def others():
        for j in range(1, at.ys):
            y = lax.rem(at.y + j, at.ys)
            yield j, y * 2 + at.core, y * 2 + 1 - at.core

    partner = at.y * 2 + 1 - at.core

    def finish_forward(sums, perturb, number):
        embedded = tokens_ref[...].astype(F32) + perturb
        out_grad = (embedded + sums.take() - target_ref[...]) * scale
        out_grad_ref[...] = out_grad
        own_grad[number] = out_grad.astype(BF16)

    emb.spread()
    emb.land()
    emb.share()
    norm(emb, at.dp, keep=True)
    loads[0].wait()
    forward(at.dp)
    loads[1].wait()
    sums = partial_out(0, landing_1)
    emb.from_core(0)
    norm(emb, partner)
    forward(partner)
    for j, same, other in others():
        emb.from_y(j)
    finish_forward(sums, adv_init * noise_ref[...], 0)
    grad = Gather(at, own_grad.at[0], grad_all, gather_sems[1])
    for j, same, other in others():
        norm(emb, same)
        forward(same)
    grad.spread()
    grad.land()
    grad.share()
    for load in late:
        load.start()

    flat_grad(grad, at.dp)
    backward(at.dp)
    sums = ScatterSum(at, outgoing, landing_2, kept, sum_sems[1])
    row_dot = jnp.zeros((rows, 1), F32)
    for k in sums.order():
        column = pl.multiple_of(sums.chunk(k) * CHUNK, CHUNK)
        value = dot_nt(hgrad[span(at.dp), :], win[pl.ds(column, CHUNK), :])
        sums.give(k, value)
        along = emb.columns_of(at.dp, column, CHUNK).astype(F32) * gain_ref[:, pl.ds(column, CHUNK)]
        row_dot = row_dot + jnp.sum(value * along, axis=1, keepdims=True)
    table_out[...] = jnp.where(lane == 0.0, row_dot, 0.0).T[:8, :]
    dots = SmallSum(at, "tensor", table_out, table_in, table_sems)
    for j, same, other in others():
        emb.from_core(j)
        norm(emb, other)
        forward(other)
    grad.from_core(0)
    flat_grad(grad, partner)
    for j, same, other in others():
        grad.from_y(j)
    scaled = gain_own * sums.take()
    row_dot = jnp.concatenate([dots.take(), jnp.zeros((rows - 8, rows), F32)], axis=0).T[:, 0:1]
    inv = inv_ref[:, :width]
    radial = own_emb[0].astype(F32) * (inv * inv * inv * (1.0 / features))
    delta = out_grad_ref[...] + inv * scaled - radial * row_dot
    square = jnp.sum(delta * delta, axis=1, keepdims=True)
    square_out[...] = jnp.broadcast_to(
        jnp.sum(onehot_ref[...] * square, axis=0, keepdims=True), (8, rows)
    )
    emb.done()
    squares = SmallSum(at, "tensor", square_out, square_in, square_sems)
    turn_in[...] = turned(normed)
    backward(partner)
    square_out_dp[...] = squares.take()
    squares = SmallSum(at, "dp", square_out_dp, square_in_dp, square_dp_sems)
    for j, same, other in others():
        flat_grad(grad, same)
        backward(same)
    counts = counting.take()
    root_mean = jnp.sqrt(squares.take() / (jnp.maximum(counts, 1.0) * features) + 1e-06)
    token_scale = jnp.sum(onehot_ref[...] * (adv_step / root_mean)[0:1, :], axis=1, keepdims=True)
    perturb = adv_init * noise_ref[...] + delta * token_scale
    perturb_ref[...] = perturb
    own_emb[1] = (tokens_ref[...].astype(F32) + perturb).astype(BF16)

    emb = Gather(at, own_emb.at[1], emb_all, gather_sems[2])
    for j, same, other in others():
        grad.from_core(j)
        flat_grad(grad, other)
        backward(other)
    turn_out[...] = turned(grad_source)
    emb.spread()
    weight_grads()
    grad.done()
    emb.land()
    emb.share()
    norm(emb, at.dp)
    forward(at.dp)
    sums = partial_out(2, landing_3)
    emb.from_core(0)
    norm(emb, partner)
    forward(partner)
    for j, same, other in others():
        emb.from_y(j)
    finish_forward(sums, perturb_ref[...], 1)
    grad = Gather(at, own_grad.at[1], grad_all, gather_sems[3])
    for j, same, other in others():
        norm(emb, same)
        forward(same)
    grad.spread()
    for j, same, other in others():
        emb.from_core(j)
        norm(emb, other)
        forward(other)
    grad.land()
    grad.share()
    turn_in[...] = turned(normed)

    flat_grad(grad, at.dp)
    backward(at.dp)
    grad.from_core(0)
    flat_grad(grad, partner)
    backward(partner)
    for j, same, other in others():
        grad.from_y(j)
        flat_grad(grad, same)
        backward(same)
    for j, same, other in others():
        grad.from_core(j)
        flat_grad(grad, other)
        backward(other)
    turn_out[...] = turned(grad_source)
    emb.done()
    grad.done()
    for load in late:
        load.wait()


def update_kernel(
    hidden, hgrad, turn_in, turn_out, acc_in, acc_out, mom_in, mom_out, own_in, own_out,
    win_hbm, wout_hbm, min_hbm, mout_hbm,
    new_min, new_mout, new_win, new_wout, sems,
):
    at = Place()
    own_cols, hidden_units = acc_in.shape
    block_cols = own_out.shape[1]
    tile = 512
    count = hidden_units // tile

    def copies(i):
        cols = pl.ds(pl.multiple_of(i * tile, tile), tile)
        return [
            pltpu.make_async_copy(new_min.at[:, cols], min_hbm.at[:, cols], sems.at[0, i]),
            pltpu.make_async_copy(new_win.at[:, cols], win_hbm.at[:, cols], sems.at[1, i]),
            pltpu.make_async_copy(new_mout.at[cols], mout_hbm.at[cols], sems.at[2, i]),
            pltpu.make_async_copy(new_wout.at[cols], wout_hbm.at[cols], sems.at[3, i]),
        ]

    offset = at.dp * own_cols - at.dp * own_cols // block_cols * block_cols

    @pl.loop(0, count)
    def _(i):
        cols = pl.ds(pl.multiple_of(i * tile, tile), tile)
        grad = acc_in[:, cols] + dot_nn(turn_in[...], hgrad[:, cols])
        moment = decay * mom_in[:, cols] + grad * (1.0 / ASCENTS)
        new_min[:, cols] = moment
        new_win[:, cols] = (own_in[:, cols].astype(F32) - learn_rate * moment).astype(BF16)
        grad = (acc_out[:, cols] + dot_nn(turn_out[...], hidden[:, cols])).T
        moment = decay * mom_out[cols, :] + grad * (1.0 / ASCENTS)
        new_mout[cols, :] = moment
        own = own_part(own_out[cols, :].astype(F32), offset, own_cols, 1)
        new_wout[cols, :] = (own - learn_rate * moment).astype(BF16)
        for copy in copies(i):
            copy.start()

    @pl.loop(0, count)
    def _(i):
        for copy in copies(i):
            copy.wait()


def room(shapes):
    size = 0
    for shape in shapes:
        if shape.memory_space == pltpu.VMEM:
            *outer, last = shape.shape
            lanes = -(-last // LANES) * LANES
            size += functools.reduce(lambda a, b: a * b, outer, lanes) * jnp.dtype(shape.dtype).itemsize
    return size + 2 * 2**20


def shards(
    tokens, init_noise, segment_ids, target, norm_gain, weight_in, weight_out, moment_in, moment_out
):
    dp_count, tensor_count = lax.axis_size("dp"), lax.axis_size("tensor")
    rows, width = tokens.shape
    features, hidden_units = weight_in.shape
    own_cols = moment_in.shape[0]
    total = rows * dp_count
    narrow = width % LANES != 0
    block_cols = max(own_cols, LANES)
    dma = pltpu.SemaphoreType.DMA
    vmem = pl.BlockSpec(memory_space=pltpu.VMEM)
    anywhere = pl.BlockSpec(memory_space=pl.ANY)
    whole = pltpu.VMEM((tensor_count, total, width) if narrow else (total, features), BF16)
    landing = pltpu.VMEM((tensor_count - 1, rows, width), BF16)
    small = pltpu.VMEM((8, rows), F32)
    over_tensor = pltpu.VMEM((tensor_count - 1, 8, rows), F32)
    over_dp = pltpu.VMEM((dp_count - 1, 8, rows), F32)

    def both(count):
        return [dma((count,)), dma((count,))]

    gather = both(gather_copies(dp_count, tensor_count))
    tensor_sems, dp_sems = both(tensor_count - 1), both(dp_count - 1)
    results = (
        pltpu.VMEM((total, hidden_units), BF16),
        pltpu.VMEM((total, hidden_units), BF16),
        pltpu.VMEM((own_cols, total), BF16),
        pltpu.VMEM((own_cols, total), BF16),
        pltpu.VMEM((own_cols, hidden_units), F32),
        pltpu.VMEM((own_cols, hidden_units), F32),
        pltpu.VMEM((own_cols, hidden_units), F32),
        pltpu.VMEM((hidden_units, own_cols), F32),
        pltpu.VMEM((own_cols, hidden_units), BF16),
        pltpu.VMEM((hidden_units, block_cols), BF16),
    )
    scratch = [
        pltpu.VMEM((features, hidden_units), BF16),
        pltpu.VMEM((hidden_units, features), BF16),
        whole,
        whole,
        pltpu.VMEM((total, features), BF16),
        pltpu.VMEM((total, features) if narrow else (16, LANES), BF16),
        pltpu.VMEM((2, rows, width), BF16),
        pltpu.VMEM((2, rows, width), BF16),
        pltpu.VMEM((rows, width), F32),
        pltpu.VMEM((rows, LANES), F32),
        pltpu.VMEM((rows, rows), F32),
        pltpu.VMEM((CHUNK // width, rows, width), F32),
        pltpu.VMEM((tensor_count, rows, width), BF16),
        landing, landing, landing,
        small, over_tensor, small, over_tensor, small, over_dp, small, over_dp,
        dma((2,)), dma((4,)),
        *gather, *gather, *gather, *gather,
        *tensor_sems, *tensor_sems, *tensor_sems,
        *tensor_sems, *tensor_sems, *dp_sems, *dp_sems,
    ]
    *kept, perturb = pl.pallas_call(
        functools.partial(
            step_kernel, scale=(rows * dp_count) ** (-0.5), features=features
        ),
        name="step",
        out_shape=(*results, jax.ShapeDtypeStruct((rows, width), F32)),
        in_specs=[vmem] * 5 + [anywhere] * 4,
        out_specs=tuple([vmem] * (len(results) + 1)),
        scratch_shapes=scratch,
        compiler_params=pltpu.CompilerParams(
            collective_id=0, has_side_effects=True, vmem_limit_bytes=room(scratch)
        ),
    )(
        tokens, init_noise, segment_ids.reshape(1, rows), target, norm_gain.reshape(1, features),
        weight_in, weight_out, moment_in, moment_out,
    )
    staged = [
        pltpu.VMEM((own_cols, hidden_units), F32),
        pltpu.VMEM((hidden_units, own_cols), F32),
        pltpu.VMEM((own_cols, hidden_units), BF16),
        pltpu.VMEM((hidden_units, own_cols), BF16),
        dma((4, hidden_units // 512)),
    ]
    new_weight_in, new_weight_out, new_moment_in, new_moment_out = pl.pallas_call(
        update_kernel,
        name="update",
        out_shape=(
            jax.ShapeDtypeStruct((own_cols, hidden_units), BF16),
            jax.ShapeDtypeStruct((hidden_units, own_cols), BF16),
            jax.ShapeDtypeStruct((own_cols, hidden_units), F32),
            jax.ShapeDtypeStruct((hidden_units, own_cols), F32),
        ),
        in_specs=[vmem] * len(kept),
        out_specs=(anywhere,) * 4,
        scratch_shapes=staged,
        compiler_params=pltpu.CompilerParams(vmem_limit_bytes=room(staged)),
    )(*kept)
    return (new_weight_in, new_weight_out, new_moment_in, new_moment_out, perturb)


def solution(mesh):
    placed = (
        P("dp", "tensor"),
        P("dp", "tensor"),
        P("dp"),
        P("dp", "tensor"),
        P(),
        P(None, "tensor"),
        P("tensor", None),
        P("dp", "tensor"),
        P("tensor", "dp"),
    )
    return jax.shard_map(
        shards,
        mesh=mesh,
        in_specs=placed,
        out_specs=(
            P("dp", "tensor"),
            P("tensor", "dp"),
            P("dp", "tensor"),
            P("tensor", "dp"),
            P("dp", "tensor"),
        ),
        check_vma=False,
    )
```

```python
import functools

import jax
import jax.numpy as jnp
from jax import lax
from jax.experimental import pallas as pl
from jax.experimental.pallas import tpu as pltpu
from jax.sharding import PartitionSpec as P

ASCENTS = 2

coeff = 0.7978845608
cubic = 0.044715
adv_init = 0.5
adv_step = 0.5
decay = 0.9
learn_rate = 0.01
LANES = 128
CHUNK = 256
TILE, TILE_WIDE = 2048, 1024
F32, BF16 = jnp.float32, jnp.bfloat16


def gelu_both(values):
    square = values * values
    half = 0.5 + 0.5 * jnp.tanh(values * (coeff + (coeff * cubic) * square))
    hidden = values * half
    slope = half + (hidden * (1.0 - half)) * (2.0 * coeff + (6.0 * coeff * cubic) * square)
    return hidden, slope


def dot_nt(left, right):
    return lax.dot_general(left, right, (((1,), (1,)), ((), ())), preferred_element_type=F32)


def dot_nn(left, right):
    return jnp.dot(left, right, preferred_element_type=F32)


class Place:
    def __init__(self):
        self.dp_count, self.tensor_count = lax.axis_size("dp"), lax.axis_size("tensor")
        self.ys, self.zs = self.dp_count // 2, self.tensor_count // 2
        self.dp, self.tensor = lax.axis_index("dp"), lax.axis_index("tensor")
        self.y, self.core = self.dp // 2, self.dp % 2
        self.z, self.x = self.tensor // 2, self.tensor % 2


def enter(at):
    barrier = pltpu.get_barrier_semaphore()
    for step in range(1, at.tensor_count):
        there = (at.dp, lax.rem(at.tensor + step, at.tensor_count))
        pl.semaphore_signal(barrier, inc=1, device_id=there, device_id_type=pl.DeviceIdType.MESH)
    for step in range(1, at.dp_count):
        there = (lax.rem(at.dp + step, at.dp_count), at.tensor)
        pl.semaphore_signal(barrier, inc=1, device_id=there, device_id_type=pl.DeviceIdType.MESH)
    pl.semaphore_wait(barrier, at.tensor_count + at.dp_count - 2)


def send(source, target, sems, number, there):
    copy = pltpu.make_async_remote_copy(
        src_ref=source,
        dst_ref=target,
        send_sem=sems[0].at[number],
        recv_sem=sems[1].at[number],
        device_id=there,
        device_id_type=pl.DeviceIdType.MESH,
    )
    copy.start()
    return copy


def gather_copies(dp_count, tensor_count):
    ys = dp_count // 2
    return tensor_count - 1 + (ys - 1) * tensor_count + ys


class Gather:
    def __init__(self, at, own_ref, whole_ref, sems):
        self.at, self.whole, self.sems = at, whole_ref, sems
        self.rows, self.cols = own_ref.shape
        self.numbers = iter(range(gather_copies(at.dp_count, at.tensor_count)))
        self.flat = len(whole_ref.shape) == 2
        self.started = []
        self.other_x = (at.dp, at.z * 2 + 1 - at.x)
        self.partner = (at.y * 2 + 1 - at.core, at.tensor)
        whole_ref[self.place(at.dp, at.tensor)] = own_ref[...]
        own = self.block(at.dp, at.tensor)
        self.along_z = [
            self.start(own_ref, own, (at.dp, lax.rem(at.z + at.zs - k, at.zs) * 2 + at.x))
            for k in range(1, at.zs)
        ]
        self.along_x = [self.start(own_ref, own, self.other_x)]
        self.along_y = {j: [] for j in range(1, at.ys)}
        self.onward(own_ref, own)

    def span(self, dp):
        return pl.ds(pl.multiple_of(dp * self.rows, self.rows), self.rows)

    def place(self, dp, tensor):
        if self.flat:
            return (self.span(dp), pl.ds(pl.multiple_of(tensor * self.cols, self.cols), self.cols))
        return (tensor, self.span(dp))

    def block(self, dp, tensor):
        return self.whole.at[self.place(dp, tensor)]

    def strip(self, dp):
        return self.whole.at[self.span(dp)] if self.flat else self.whole.at[:, self.span(dp)]

    def start(self, source, target, there):
        copy = send(source, target, self.sems, next(self.numbers), there)
        self.started.append(copy)
        return copy

    def onward(self, source, block):
        at = self.at
        for j, copies in self.along_y.items():
            there = (lax.rem(at.y + at.ys - j, at.ys) * 2 + at.core, at.tensor)
            copies.append(self.start(source, block, there))

    def spread(self):
        at = self.at
        for k in range(1, at.zs):
            self.along_z[k - 1].wait_recv()
            block = self.block(at.dp, lax.rem(at.z + k, at.zs) * 2 + at.x)
            self.along_x.append(self.start(block, block, self.other_x))
            self.onward(block, block)

    def land(self):
        at = self.at
        for k, copy in enumerate(self.along_x):
            copy.wait_recv()
            block = self.block(at.dp, lax.rem(at.z + k, at.zs) * 2 + 1 - at.x)
            self.onward(block, block)
        strip = self.strip(at.dp)
        self.to_core = {0: self.start(strip, strip, self.partner)}

    def from_y(self, j):
        at = self.at
        for copy in self.along_y[j]:
            copy.wait_recv()
        strip = self.strip(lax.rem(at.y + j, at.ys) * 2 + at.core)
        self.to_core[j] = self.start(strip, strip, self.partner)

    def from_core(self, j):
        self.to_core[j].wait_recv()

    def done(self):
        for copy in self.started:
            copy.wait_send()

    def row_block(self, dp):
        if self.flat:
            return self.whole[self.span(dp), :]
        return jnp.concatenate(
            [self.whole[t, self.span(dp), :] for t in range(self.at.tensor_count)], axis=1
        )

    def columns_of(self, dp, column, width):
        if self.flat:
            return self.whole[self.span(dp), pl.ds(pl.multiple_of(column, width), width)]
        first = column // self.cols
        return jnp.concatenate(
            [self.whole[first + i, self.span(dp), :] for i in range(width // self.cols)], axis=1
        )


class ScatterSum:
    def __init__(self, at, outgoing, landing, kept, sems):
        self.at, self.outgoing, self.landing, self.kept, self.sems = (
            at, outgoing, landing, kept, sems
        )
        self.cols = outgoing.shape[2]
        self.group = CHUNK // self.cols
        self.chunks = at.tensor_count // self.group
        self.inner = at.tensor % self.group
        self.copies = {}

    def order(self):
        half = self.chunks // 2
        return sorted(range(self.chunks), key=lambda k: (k == 0, abs(k - half)))

    def chunk(self, k):
        return lax.rem(self.at.tensor // self.group + k, self.chunks)

    def give(self, k, value):
        first = self.chunk(k) * self.group
        for i in range(self.group):
            part = value[:, i * self.cols:(i + 1) * self.cols]
            self.outgoing[first + i] = part.astype(BF16)
            if k == 0:
                self.kept[i] = part
        for j in range(self.group):
            label = k * self.group + j
            if label:
                there = first + lax.rem(self.inner + j, self.group)
                self.copies[label] = send(
                    self.outgoing.at[there], self.landing.at[label - 1], self.sems, label - 1,
                    (self.at.dp, there),
                )

    def take(self):
        value = self.kept[self.inner]
        for label, copy in self.copies.items():
            copy.wait_recv()
            value = value + self.landing[label - 1].astype(F32)
        for copy in self.copies.values():
            copy.wait_send()
        return value


class SmallSum:
    def __init__(self, at, axis, out, landing, sems):
        count = at.dp_count if axis == "dp" else at.tensor_count
        self.out, self.landing, self.copies = out, landing, []
        for step in range(1, count):
            if axis == "dp":
                there = (lax.rem(at.dp + step, count), at.tensor)
            else:
                there = (at.dp, lax.rem(at.tensor + step, count))
            self.copies.append(send(out, landing.at[step - 1], sems, step - 1, there))

    def take(self):
        value = self.out[...]
        for step, copy in enumerate(self.copies):
            copy.wait_recv()
            value = value + self.landing[step]
        for copy in self.copies:
            copy.wait_send()
        return value


def own_part(value, offset, size, axis):
    parts = [lax.slice_in_dim(value, s, s + size, axis=axis) for s in range(0, value.shape[axis], size)]
    result = parts[0]
    for i, part in enumerate(parts[1:], 1):
        result = jnp.where(offset == i * size, part, result)
    return result


def turned(at, source, own_cols):
    block = max(own_cols, LANES)
    start = at.dp * own_cols // block * block
    value = source[:, pl.ds(pl.multiple_of(start, block), block)].astype(F32).T
    return own_part(value, at.dp * own_cols - start, own_cols, 0).astype(BF16)


def tiles(body, size, tile, part=0, parts=1):
    share = size // tile // parts

    @pl.loop(part * share, (part + 1) * share)
    def _(i):
        body(pl.ds(pl.multiple_of(i * tile, tile), tile))


def backward_tile(grad_flat, wout_t, hgrad, span, cols):
    value = dot_nn(grad_flat[span, :], wout_t[:, cols])
    hgrad[span, cols] = (value * hgrad[span, cols].astype(F32)).astype(BF16)


def step_kernel(
    tokens_hbm, noise_hbm, ids_hbm, target_hbm, gain_hbm, win_hbm, wout_hbm, min_hbm, mout_hbm,
    hidden, hgrad, turn_in, mom_in, mom_out, own_in, own_out, wout_t, grad_flat, perturb_ref,
    tokens_ref, noise_ref, ids_ref, target_ref, gain_ref,
    win, wout, emb_all, grad_3d, normed, own_emb, own_grad, out_grad_ref, inv_ref,
    onehot_ref, kept, outgoing, landing_1, landing_2, landing_3,
    table_out, table_in, square_out, square_in, square_out_dp, square_in_dp, count_out, count_in,
    load_sems, late_sems, *sems, scale, features,
):
    at = Place()
    rows, width = tokens_ref.shape
    hidden_units = win.shape[1]
    own_cols = mom_in.shape[0]
    pairs = [(sems[2 * i], sems[2 * i + 1]) for i in range(len(sems) // 2)]
    gather_sems, sum_sems = pairs[:4], pairs[4:7]
    table_sems, square_sems, square_dp_sems, count_sems = pairs[7:11]
    narrow = len(emb_all.shape) == 3
    grad_all = grad_3d if narrow else grad_flat

    small = [(tokens_hbm, tokens_ref), (noise_hbm, noise_ref)]
    small += [(ids_hbm, ids_ref), (gain_hbm, gain_ref), (target_hbm, target_ref)]
    loads = [
        pltpu.make_async_copy(source, target, load_sems.at[i])
        for i, (source, target) in enumerate(small + [(wout_hbm, wout), (win_hbm, win)])
    ]
    for load in loads:
        load.start()
    block_cols = own_out.shape[1]
    first_col = at.dp * own_cols // block_cols * block_cols
    late = [
        pltpu.make_async_copy(
            win_hbm.at[pl.ds(pl.multiple_of(at.dp * own_cols, own_cols), own_cols)], own_in,
            late_sems.at[0],
        ),
        pltpu.make_async_copy(
            wout_hbm.at[:, pl.ds(pl.multiple_of(first_col, block_cols), block_cols)], own_out,
            late_sems.at[1],
        ),
        pltpu.make_async_copy(min_hbm, mom_in, late_sems.at[2]),
        pltpu.make_async_copy(mout_hbm, mom_out, late_sems.at[3]),
    ]
    for load in loads[:5]:
        load.wait()
    own_emb[0] = (tokens_ref[...].astype(F32) + adv_init * noise_ref[...]).astype(BF16)
    enter(at)
    emb = Gather(at, own_emb.at[0], emb_all, gather_sems[0])

    lane = lax.broadcasted_iota(jnp.int32, (rows, rows), 1).astype(F32)
    ids = jnp.broadcast_to(ids_ref[...].astype(F32), (rows, rows)).T
    onehot = (ids == lane).astype(F32)
    onehot_ref[...] = onehot
    count_out[...] = jnp.broadcast_to(jnp.sum(onehot, axis=0, keepdims=True), (8, rows))
    counting = SmallSum(at, "dp", count_out, count_in, count_sems)
    group = max(width, LANES)
    first = at.tensor * width // group * group
    gain_own = own_part(
        gain_ref[:, pl.ds(pl.multiple_of(first, group), group)], at.tensor * width - first, width, 1
    )

    def span(dp, count=1):
        return pl.ds(pl.multiple_of(dp * rows, count * rows), count * rows)

    def norm(gather, dp, keep=False):
        block = gather.row_block(dp).astype(F32)
        inv = lax.rsqrt(jnp.mean(block * block, axis=1, keepdims=True) + 1e-06)
        normed[span(dp), :] = (block * inv * gain_ref[...]).astype(BF16)
        if keep:
            inv_ref[...] = jnp.broadcast_to(inv, inv_ref.shape)

    def forward(dp, count=1, part=0, parts=1):
        def body(cols):
            value, slope = gelu_both(dot_nn(normed[span(dp, count), :], win[:, cols]))
            hidden[span(dp, count), cols] = value.astype(BF16)
            hgrad[span(dp, count), cols] = slope.astype(BF16)

        tiles(body, hidden_units, TILE if count == 1 else TILE_WIDE, part, parts)

    def flat_grad(gather, dp):
        if narrow:
            grad_flat[span(dp), :] = gather.row_block(dp)

    def backward(dp, count=1, part=0, parts=1):
        body = functools.partial(backward_tile, grad_flat, wout_t, hgrad, span(dp, count))
        tiles(body, hidden_units, TILE if count == 1 else TILE_WIDE, part, parts)

    def partial_out(number, landing):
        sums = ScatterSum(at, outgoing, landing, kept, sum_sems[number])
        for k in sums.order():
            column = pl.multiple_of(sums.chunk(k) * CHUNK, CHUNK)
            sums.give(k, dot_nn(hidden[span(at.dp), :], wout[:, pl.ds(column, CHUNK)]))
        return sums

    partner = at.y * 2 + 1 - at.core
    planes = [(j, lax.rem(at.y + j, at.ys) * 2) for j in range(1, at.ys)]

    def arrive(gather, then):
        for j, plane in planes:
            gather.from_y(j)
        for j, plane in planes:
            gather.from_core(j)
            then(gather, plane)
            then(gather, plane + 1)

    def forward_planes(part):
        for j, plane in planes:
            forward(plane, 2, part, 2)

    def backward_planes(part):
        for j, plane in planes:
            backward(plane, 2, part, 2)

    def finish_forward(sums, perturb, number):
        embedded = tokens_ref[...].astype(F32) + perturb
        out_grad = (embedded + sums.take() - target_ref[...]) * scale
        out_grad_ref[...] = out_grad
        own_grad[number] = out_grad.astype(BF16)

    def turn_weights(part):
        def body(cols):
            wout_t[:, cols] = wout[cols, :].T

        tiles(body, hidden_units, 512, part, 2)

    loads[5].wait()
    turn_weights(0)
    emb.spread()
    turn_weights(1)
    emb.land()
    norm(emb, at.dp, keep=True)
    loads[6].wait()
    forward(at.dp)
    for load in late:
        load.start()
    sums = partial_out(0, landing_1)
    emb.from_core(0)
    norm(emb, partner)
    forward(partner)
    arrive(emb, norm)
    forward_planes(0)
    finish_forward(sums, adv_init * noise_ref[...], 0)
    grad = Gather(at, own_grad.at[0], grad_all, gather_sems[1])
    forward_planes(1)
    turn_in[...] = turned(at, normed, own_cols)
    grad.spread()
    grad.land()

    flat_grad(grad, at.dp)
    backward(at.dp)
    sums = ScatterSum(at, outgoing, landing_2, kept, sum_sems[1])
    row_dot = jnp.zeros((rows, 1), F32)
    for k in sums.order():
        column = pl.multiple_of(sums.chunk(k) * CHUNK, CHUNK)
        value = dot_nt(hgrad[span(at.dp), :], win[pl.ds(column, CHUNK), :])
        sums.give(k, value)
        along = emb.columns_of(at.dp, column, CHUNK).astype(F32) * gain_ref[:, pl.ds(column, CHUNK)]
        row_dot = row_dot + jnp.sum(value * along, axis=1, keepdims=True)
    table_out[...] = jnp.where(lane == 0.0, row_dot, 0.0).T[:8, :]
    dots = SmallSum(at, "tensor", table_out, table_in, table_sems)
    grad.from_core(0)
    flat_grad(grad, partner)
    backward(partner)
    arrive(grad, flat_grad)
    backward_planes(0)
    scaled = gain_own * sums.take()
    row_dot = jnp.concatenate([dots.take(), jnp.zeros((rows - 8, rows), F32)], axis=0).T[:, 0:1]
    inv = inv_ref[:, :width]
    radial = own_emb[0].astype(F32) * (inv * inv * inv * (1.0 / features))
    delta = out_grad_ref[...] + inv * scaled - radial * row_dot
    square = jnp.sum(delta * delta, axis=1, keepdims=True)
    square_out[...] = jnp.broadcast_to(
        jnp.sum(onehot_ref[...] * square, axis=0, keepdims=True), (8, rows)
    )
    out_grad_ref[...] = delta
    emb.done()
    squares = SmallSum(at, "tensor", square_out, square_in, square_sems)
    backward_planes(1)
    square_out_dp[...] = squares.take()
    squares = SmallSum(at, "dp", square_out_dp, square_in_dp, square_dp_sems)
    turn_out = turned(at, grad_flat, own_cols)
    counts = counting.take()
    root_mean = jnp.sqrt(squares.take() / (jnp.maximum(counts, 1.0) * features) + 1e-06)
    token_scale = jnp.sum(onehot_ref[...] * (adv_step / root_mean)[0:1, :], axis=1, keepdims=True)
    perturb = adv_init * noise_ref[...] + out_grad_ref[...] * token_scale
    perturb_ref[...] = perturb
    own_emb[1] = (tokens_ref[...].astype(F32) + perturb).astype(BF16)

    emb = Gather(at, own_emb.at[1], emb_all, gather_sems[2])
    for load in late:
        load.wait()

    def moment_in_tile(cols):
        gradient = dot_nn(turn_in[...], hgrad[:, cols])
        mom_in[:, cols] = decay * mom_in[:, cols] + gradient * (1.0 / ASCENTS)

    def moment_out_tile(cols):
        gradient = dot_nn(turn_out, hidden[:, cols]).T
        mom_out[cols, :] = decay * mom_out[cols, :] + gradient * (1.0 / ASCENTS)

    tiles(moment_in_tile, hidden_units, 512)
    emb.spread()
    tiles(moment_out_tile, hidden_units, 512)
    grad.done()
    emb.land()
    norm(emb, at.dp)
    forward(at.dp)
    sums = partial_out(2, landing_3)
    emb.from_core(0)
    norm(emb, partner)
    forward(partner)
    arrive(emb, norm)
    forward_planes(0)
    finish_forward(sums, perturb_ref[...], 1)
    grad = Gather(at, own_grad.at[1], grad_all, gather_sems[3])
    forward_planes(1)
    turn_in[...] = turned(at, normed, own_cols)
    grad.spread()
    grad.land()

    flat_grad(grad, at.dp)
    backward(at.dp)
    grad.from_core(0)
    flat_grad(grad, partner)
    backward(partner)
    arrive(grad, flat_grad)
    emb.done()
    grad.done()


def update_kernel(
    hidden, hgrad, turn_in, mom_in, mom_out, own_in, own_out, wout_t, grad_flat, perturb_ref,
    win_hbm, wout_hbm, min_hbm, mout_hbm, perturb_hbm,
    new_min, new_mout, new_win, new_wout, turn_out, perturb_sem, sems,
):
    at = Place()
    own_cols, hidden_units = mom_in.shape
    pair = perturb_ref.shape[0] * 2
    block_cols = own_out.shape[1]
    tile = 1024
    count = hidden_units // tile
    perturb_out = pltpu.make_async_copy(perturb_ref, perturb_hbm, perturb_sem)
    perturb_out.start()
    turn_out[...] = turned(at, grad_flat, own_cols)

    def copies(i):
        cols = pl.ds(pl.multiple_of(i * tile, tile), tile)
        return [
            pltpu.make_async_copy(new_min.at[:, cols], min_hbm.at[:, cols], sems.at[0, i]),
            pltpu.make_async_copy(new_win.at[:, cols], win_hbm.at[:, cols], sems.at[1, i]),
            pltpu.make_async_copy(new_mout.at[cols], mout_hbm.at[cols], sems.at[2, i]),
            pltpu.make_async_copy(new_wout.at[cols], wout_hbm.at[cols], sems.at[3, i]),
        ]

    offset = at.dp * own_cols - at.dp * own_cols // block_cols * block_cols

    @pl.loop(0, count)
    def _(i):
        cols = pl.ds(pl.multiple_of(i * tile, tile), tile)
        gradient = dot_nn(turn_out[...], hidden[:, cols]).T
        moment = decay_rest(mom_out[cols, :], gradient)
        new_mout[cols, :] = moment
        own = own_part(own_out[cols, :].astype(F32), offset, own_cols, 1)
        new_wout[cols, :] = (own - learn_rate * moment).astype(BF16)
        for j in range(1, at.ys):
            start = lax.rem(at.y + j, at.ys) * pair
            backward_tile(grad_flat, wout_t, hgrad, pl.ds(pl.multiple_of(start, pair), pair), cols)
        gradient = dot_nn(turn_in[...], hgrad[:, cols])
        moment = decay_rest(mom_in[:, cols], gradient)
        new_min[:, cols] = moment
        new_win[:, cols] = (own_in[:, cols].astype(F32) - learn_rate * moment).astype(BF16)
        for copy in copies(i):
            copy.start()

    @pl.loop(0, count)
    def _(i):
        for copy in copies(i):
            copy.wait()

    perturb_out.wait()


def decay_rest(moment, gradient):
    return moment + gradient * (1.0 / ASCENTS)


def room(shapes):
    size = 0
    for shape in shapes:
        if shape.memory_space == pltpu.VMEM:
            *outer, last = shape.shape
            lanes = -(-last // LANES) * LANES
            size += functools.reduce(lambda a, b: a * b, outer, lanes) * jnp.dtype(shape.dtype).itemsize
    return size + 4 * 2**20


def shards(
    tokens, init_noise, segment_ids, target, norm_gain, weight_in, weight_out, moment_in, moment_out
):
    dp_count, tensor_count = lax.axis_size("dp"), lax.axis_size("tensor")
    rows, width = tokens.shape
    features, hidden_units = weight_in.shape
    own_cols = moment_in.shape[0]
    total = rows * dp_count
    narrow = width % LANES != 0
    block_cols = max(own_cols, LANES)
    dma = pltpu.SemaphoreType.DMA
    vmem = pl.BlockSpec(memory_space=pltpu.VMEM)
    anywhere = pl.BlockSpec(memory_space=pltpu.HBM)
    whole = pltpu.VMEM((tensor_count, total, width) if narrow else (total, features), BF16)
    landing = pltpu.VMEM((tensor_count - 1, rows, width), BF16)
    small = pltpu.VMEM((8, rows), F32)
    over_tensor = pltpu.VMEM((tensor_count - 1, 8, rows), F32)
    over_dp = pltpu.VMEM((dp_count - 1, 8, rows), F32)

    def both(count):
        return [dma((count,)), dma((count,))]

    gather = both(gather_copies(dp_count, tensor_count))
    tensor_sems, dp_sems = both(tensor_count - 1), both(dp_count - 1)
    results = (
        pltpu.VMEM((total, hidden_units), BF16),
        pltpu.VMEM((total, hidden_units), BF16),
        pltpu.VMEM((own_cols, total), BF16),
        pltpu.VMEM((own_cols, hidden_units), F32),
        pltpu.VMEM((hidden_units, own_cols), F32),
        pltpu.VMEM((own_cols, hidden_units), BF16),
        pltpu.VMEM((hidden_units, block_cols), BF16),
        pltpu.VMEM((features, hidden_units), BF16),
        pltpu.VMEM((total, features), BF16),
        pltpu.VMEM((rows, width), F32),
    )
    scratch = [
        pltpu.VMEM((rows, width), BF16),
        pltpu.VMEM((rows, width), F32),
        pltpu.VMEM((1, rows), jnp.int32),
        pltpu.VMEM((rows, width), F32),
        pltpu.VMEM((1, features), F32),
        pltpu.VMEM((features, hidden_units), BF16),
        pltpu.VMEM((hidden_units, features), BF16),
        whole,
        whole if narrow else pltpu.VMEM((16, LANES), BF16),
        pltpu.VMEM((total, features), BF16),
        pltpu.VMEM((2, rows, width), BF16),
        pltpu.VMEM((2, rows, width), BF16),
        pltpu.VMEM((rows, width), F32),
        pltpu.VMEM((rows, LANES), F32),
        pltpu.VMEM((rows, rows), F32),
        pltpu.VMEM((CHUNK // width, rows, width), F32),
        pltpu.VMEM((tensor_count, rows, width), BF16),
        landing, landing, landing,
        small, over_tensor, small, over_tensor, small, over_dp, small, over_dp,
        dma((7,)), dma((4,)),
        *gather, *gather, *gather, *gather,
        *tensor_sems, *tensor_sems, *tensor_sems,
        *tensor_sems, *tensor_sems, *dp_sems, *dp_sems,
    ]
    kept = pl.pallas_call(
        functools.partial(
            step_kernel, scale=(rows * dp_count) ** (-0.5), features=features
        ),
        name="step",
        out_shape=results,
        in_specs=[anywhere] * 9,
        out_specs=(vmem,) * len(results),
        scratch_shapes=scratch,
        compiler_params=pltpu.CompilerParams(
            collective_id=0, has_side_effects=True, vmem_limit_bytes=room(scratch)
        ),
    )(
        *(
            pltpu.with_memory_space_constraint(array, pltpu.HBM)
            for array in (
                tokens, init_noise, segment_ids.reshape(1, rows), target,
                norm_gain.reshape(1, features), weight_in, weight_out, moment_in, moment_out,
            )
        )
    )
    staged = [
        pltpu.VMEM((own_cols, hidden_units), F32),
        pltpu.VMEM((hidden_units, own_cols), F32),
        pltpu.VMEM((own_cols, hidden_units), BF16),
        pltpu.VMEM((hidden_units, own_cols), BF16),
        pltpu.VMEM((own_cols, total), BF16),
        dma(()),
        dma((4, hidden_units // 1024)),
    ]
    return pl.pallas_call(
        update_kernel,
        name="update",
        out_shape=(
            jax.ShapeDtypeStruct((own_cols, hidden_units), BF16),
            jax.ShapeDtypeStruct((hidden_units, own_cols), BF16),
            jax.ShapeDtypeStruct((own_cols, hidden_units), F32),
            jax.ShapeDtypeStruct((hidden_units, own_cols), F32),
            jax.ShapeDtypeStruct((rows, width), F32),
        ),
        in_specs=[vmem] * len(kept),
        out_specs=(anywhere,) * 5,
        scratch_shapes=staged,
        compiler_params=pltpu.CompilerParams(vmem_limit_bytes=max(room(staged), room(scratch))),
    )(*kept)


def solution(mesh):
    placed = (
        P("dp", "tensor"),
        P("dp", "tensor"),
        P("dp"),
        P("dp", "tensor"),
        P(),
        P(None, "tensor"),
        P("tensor", None),
        P("dp", "tensor"),
        P("tensor", "dp"),
    )
    return jax.shard_map(
        shards,
        mesh=mesh,
        in_specs=placed,
        out_specs=(
            P("dp", "tensor"),
            P("tensor", "dp"),
            P("dp", "tensor"),
            P("tensor", "dp"),
            P("dp", "tensor"),
        ),
        check_vma=False,
    )
```

```python
import functools

import jax
import jax.numpy as jnp
from jax import lax
from jax.experimental import pallas as pl
from jax.experimental.pallas import tpu as pltpu
from jax.sharding import PartitionSpec as P

ASCENTS = 2

coeff = 0.7978845608
cubic = 0.044715
adv_init = 0.5
adv_step = 0.5
decay = 0.9
learn_rate = 0.01
LANES = 128
CHUNK = 256
TILE, TILE_WIDE = 2048, 1024
F32, BF16 = jnp.float32, jnp.bfloat16


def gelu_both(values):
    square = values * values
    half = 0.5 + 0.5 * jnp.tanh(values * (coeff + (coeff * cubic) * square))
    hidden = values * half
    slope = half + (hidden * (1.0 - half)) * (2.0 * coeff + (6.0 * coeff * cubic) * square)
    return hidden, slope


def dot_nt(left, right):
    return lax.dot_general(left, right, (((1,), (1,)), ((), ())), preferred_element_type=F32)


def dot_nn(left, right):
    return jnp.dot(left, right, preferred_element_type=F32)


class Place:
    def __init__(self):
        self.dp_count, self.tensor_count = lax.axis_size("dp"), lax.axis_size("tensor")
        self.ys, self.zs = self.dp_count // 2, self.tensor_count // 2
        self.dp, self.tensor = lax.axis_index("dp"), lax.axis_index("tensor")
        self.y, self.core = self.dp // 2, self.dp % 2
        self.z, self.x = self.tensor // 2, self.tensor % 2


def enter(at):
    barrier = pltpu.get_barrier_semaphore()
    for step in range(1, at.tensor_count):
        there = (at.dp, lax.rem(at.tensor + step, at.tensor_count))
        pl.semaphore_signal(barrier, inc=1, device_id=there, device_id_type=pl.DeviceIdType.MESH)
    for step in range(1, at.dp_count):
        there = (lax.rem(at.dp + step, at.dp_count), at.tensor)
        pl.semaphore_signal(barrier, inc=1, device_id=there, device_id_type=pl.DeviceIdType.MESH)


def entered(at):
    pl.semaphore_wait(pltpu.get_barrier_semaphore(), at.tensor_count + at.dp_count - 2)


def send(source, target, sems, number, there, landed=None):
    copy = pltpu.make_async_remote_copy(
        src_ref=source,
        dst_ref=target,
        send_sem=sems[0].at[number],
        recv_sem=sems[1].at[number if landed is None else landed],
        device_id=there,
        device_id_type=pl.DeviceIdType.MESH,
    )
    copy.start()
    return copy


def gather_copies(dp_count, tensor_count):
    ys = dp_count // 2
    return tensor_count + (ys - 1) * tensor_count + ys


def pack(block):
    parts = max(1, LANES // block.shape[1])
    size = block.shape[0] // parts
    return jnp.concatenate([block[i * size:(i + 1) * size] for i in range(parts)], axis=1)


def unpack(block, width):
    return jnp.concatenate(
        [block[:, i:i + width] for i in range(0, block.shape[1], width)], axis=0
    )


class Gather:
    def __init__(self, at, own_ref, whole_ref, sems):
        self.at, self.whole, self.sems = at, whole_ref, sems
        self.rows, self.cols = own_ref.shape
        self.numbers = iter(range(at.zs, gather_copies(at.dp_count, at.tensor_count)))
        self.flat = len(whole_ref.shape) == 2
        self.started = []
        self.other_x = (at.dp, at.z * 2 + 1 - at.x)
        self.partner = (at.y * 2 + 1 - at.core, at.tensor)
        whole_ref[self.place(at.dp, at.tensor)] = own_ref[...]
        own = self.block(at.dp, at.tensor)
        for m in range(at.zs - 1):
            there = (at.dp, self.across(m) * 2 + at.x)
            self.started.append(send(own_ref, own, sems, m, there, landed=at.z))
        self.along_x = [self.start(own_ref, own, self.other_x)]
        self.along_y = {j: [] for j in range(1, at.ys)}
        self.onward(own_ref, own)

    def span(self, dp):
        return pl.ds(pl.multiple_of(dp * self.rows, self.rows), self.rows)

    def place(self, dp, tensor):
        if self.flat:
            return (self.span(dp), pl.ds(pl.multiple_of(tensor * self.cols, self.cols), self.cols))
        return (tensor, self.span(dp))

    def block(self, dp, tensor):
        return self.whole.at[self.place(dp, tensor)]

    def strip(self, dp):
        return self.whole.at[self.span(dp)] if self.flat else self.whole.at[:, self.span(dp)]

    def start(self, source, target, there):
        copy = send(source, target, self.sems, next(self.numbers), there)
        self.started.append(copy)
        return copy

    def across(self, m):
        at = self.at
        upper = at.z // (at.zs // 2)
        last = at.zs - 1 - m
        down = last - (at.z - last + at.zs) // at.zs
        up = m + (m - at.z + at.zs) // at.zs
        return upper * up + (1 - upper) * down

    def nearest(self):
        return [self.across(m) for m in reversed(range(self.at.zs - 1))]

    def onward(self, source, block):
        at = self.at
        for j, copies in self.along_y.items():
            there = (lax.rem(at.y + at.ys - j, at.ys) * 2 + at.core, at.tensor)
            copies.append(self.start(source, block, there))

    def spread(self):
        at = self.at
        for z in self.nearest():
            block = self.block(at.dp, z * 2 + at.x)
            pltpu.make_async_remote_copy(
                src_ref=block,
                dst_ref=block,
                send_sem=self.sems[0].at[0],
                recv_sem=self.sems[1].at[z],
                device_id=self.other_x,
                device_id_type=pl.DeviceIdType.MESH,
            ).wait_recv()
            self.along_x.append(self.start(block, block, self.other_x))
            self.onward(block, block)

    def land(self):
        at = self.at
        for z, copy in zip([at.z] + self.nearest(), self.along_x):
            copy.wait_recv()
            block = self.block(at.dp, z * 2 + 1 - at.x)
            self.onward(block, block)
        strip = self.strip(at.dp)
        self.to_core = {0: self.start(strip, strip, self.partner)}

    def from_y(self, j):
        at = self.at
        for copy in self.along_y[j]:
            copy.wait_recv()
        strip = self.strip(lax.rem(at.y + j, at.ys) * 2 + at.core)
        self.to_core[j] = self.start(strip, strip, self.partner)

    def from_core(self, j):
        self.to_core[j].wait_recv()

    def done(self):
        for copy in self.started:
            copy.wait_send()

    def row_block(self, dp, width):
        if self.flat:
            return self.whole[self.span(dp), :]
        return jnp.concatenate(
            [unpack(self.whole[t, self.span(dp), :], width) for t in range(self.at.tensor_count)],
            axis=1,
        )


class ScatterSum:
    def __init__(self, at, outgoing, landing, kept, sems):
        self.at, self.outgoing, self.landing, self.kept, self.sems = (
            at, outgoing, landing, kept, sems
        )
        self.cols = outgoing.shape[2]
        self.group = CHUNK // self.cols
        self.chunks = at.tensor_count // self.group
        self.inner = at.tensor % self.group
        self.copies = {}

    def order(self):
        half = self.chunks // 2
        return sorted(range(self.chunks), key=lambda k: (k == 0, abs(k - half)))

    def chunk(self, k):
        return lax.rem(self.at.tensor // self.group + k, self.chunks)

    def give(self, k, value):
        first = self.chunk(k) * self.group
        for i in range(self.group):
            part = value[:, i * self.cols:(i + 1) * self.cols]
            self.outgoing[first + i] = part.astype(BF16)
            if k == 0:
                self.kept[i] = part
        for j in range(self.group):
            label = k * self.group + j
            if label:
                there = first + lax.rem(self.inner + j, self.group)
                self.copies[label] = send(
                    self.outgoing.at[there], self.landing.at[label - 1], self.sems, label - 1,
                    (self.at.dp, there),
                )

    def take(self):
        value = self.kept[self.inner]
        for label, copy in self.copies.items():
            copy.wait_recv()
            value = value + self.landing[label - 1].astype(F32)
        for copy in self.copies.values():
            copy.wait_send()
        return value


class SmallSum:
    def __init__(self, at, axis, out, landing, sems):
        count = at.dp_count if axis == "dp" else at.tensor_count
        self.out, self.landing, self.copies = out, landing, []
        for step in range(1, count):
            if axis == "dp":
                there = (lax.rem(at.dp + step, count), at.tensor)
            else:
                there = (at.dp, lax.rem(at.tensor + step, count))
            self.copies.append(send(out, landing.at[step - 1], sems, step - 1, there))

    def take(self):
        value = self.out[...]
        for step, copy in enumerate(self.copies):
            copy.wait_recv()
            value = value + self.landing[step]
        for copy in self.copies:
            copy.wait_send()
        return value


def own_part(value, offset, size, axis):
    parts = [lax.slice_in_dim(value, s, s + size, axis=axis) for s in range(0, value.shape[axis], size)]
    result = parts[0]
    for i, part in enumerate(parts[1:], 1):
        result = jnp.where(offset == i * size, part, result)
    return result


def turned(at, source, own_cols):
    block = max(own_cols, LANES)
    start = at.dp * own_cols // block * block
    value = source[:, pl.ds(pl.multiple_of(start, block), block)].astype(F32).T
    return own_part(value, at.dp * own_cols - start, own_cols, 0).astype(BF16)


def tiles(body, size, tile, part=0, parts=1):
    share = size // tile // parts

    @pl.loop(part * share, (part + 1) * share)
    def _(i):
        body(pl.ds(pl.multiple_of(i * tile, tile), tile))


def tile_of(at, tile):
    return tile if at.ys <= 2 else CHUNK


def backward_tile(grad_flat, wout_t, hgrad, span, cols):
    value = dot_nn(grad_flat[span, :], wout_t[:, cols])
    hgrad[span, cols] = (value * hgrad[span, cols].astype(F32)).astype(BF16)


def step_kernel(
    tokens_hbm, noise_hbm, ids_hbm, target_hbm, gain_hbm, win_hbm, wout_hbm, min_hbm, mout_hbm,
    hidden, hgrad, turn_in, mom_in, mom_out, own_in, own_out, wout_t, grad_flat, perturb_ref,
    tokens_ref, noise_ref, ids_ref, target_ref, gain_ref,
    win, wout, emb_all, emb_kept, delta_whole, grad_3d, normed, own_emb, own_grad, out_grad_ref, inv_ref,
    onehot_ref, scale_ref, kept, outgoing, landing_1, landing_2, landing_3,
    table_out, table_in, square_out, square_in, square_out_dp, square_in_dp, count_out, count_in,
    load_sems, late_sems, *sems, scale, features,
):
    at = Place()
    rows, width = tokens_ref.shape
    hidden_units = win.shape[1]
    own_cols = mom_in.shape[0]
    pairs = [(sems[2 * i], sems[2 * i + 1]) for i in range(len(sems) // 2)]
    gather_sems, sum_sems = pairs[:4], pairs[4:7]
    table_sems, square_sems, square_dp_sems, count_sems = pairs[7:11]
    narrow = len(emb_all.shape) == 3
    grad_all = grad_3d if narrow else grad_flat
    emb_flat = emb_kept if narrow else emb_all
    delta_all = emb_all if narrow else delta_whole

    small = [(tokens_hbm, tokens_ref), (noise_hbm, noise_ref)]
    small += [(ids_hbm, ids_ref), (gain_hbm, gain_ref), (target_hbm, target_ref)]
    loads = [
        pltpu.make_async_copy(source, target, load_sems.at[i])
        for i, (source, target) in enumerate(small + [(wout_hbm, wout), (win_hbm, win)])
    ]
    for load in loads:
        load.start()
    block_cols = own_out.shape[1]
    first_col = at.dp * own_cols // block_cols * block_cols
    late = [
        pltpu.make_async_copy(
            win_hbm.at[pl.ds(pl.multiple_of(at.dp * own_cols, own_cols), own_cols)], own_in,
            late_sems.at[0],
        ),
        pltpu.make_async_copy(
            wout_hbm.at[:, pl.ds(pl.multiple_of(first_col, block_cols), block_cols)], own_out,
            late_sems.at[1],
        ),
        pltpu.make_async_copy(min_hbm, mom_in, late_sems.at[2]),
        pltpu.make_async_copy(mout_hbm, mom_out, late_sems.at[3]),
    ]
    enter(at)
    for load in loads[:5]:
        load.wait()
    def first_emb():
        return (tokens_ref[...].astype(F32) + adv_init * noise_ref[...]).astype(BF16)

    own_emb[0] = pack(first_emb())
    entered(at)
    emb = Gather(at, own_emb.at[0], emb_all, gather_sems[0])

    lane = lax.broadcasted_iota(jnp.int32, (rows, rows), 1).astype(F32)

    def members(ids):
        return (jnp.broadcast_to(ids, (rows, rows)).T == lane).astype(F32)

    onehot_ref[at.dp] = members(ids_ref[...].astype(F32))
    count_out[0:4, :] = jnp.broadcast_to(
        jnp.sum(onehot_ref[at.dp], axis=0, keepdims=True), (4, rows)
    )
    count_out[4:8, :] = jnp.broadcast_to(ids_ref[...].astype(F32), (4, rows))
    counting = SmallSum(at, "dp", count_out, count_in, count_sems)
    group = max(width, LANES)
    first = at.tensor * width // group * group
    gain_own = own_part(
        gain_ref[:, pl.ds(pl.multiple_of(first, group), group)], at.tensor * width - first, width, 1
    )

    def span(dp, count=1):
        return pl.ds(pl.multiple_of(dp * rows, count * rows), count * rows)

    def norm(gather, dp, keep=False):
        block = gather.row_block(dp, width)
        if narrow:
            emb_flat[span(dp), :] = block
        norm_rows(dp, block.astype(F32), keep)

    def norm_moved(gather, dp):
        step = jnp.sum(onehot_ref[dp] * scale_ref[0:1, :], axis=1, keepdims=True)
        moved = emb_flat[span(dp), :].astype(F32) + step * gather.row_block(dp, width).astype(F32)
        norm_rows(dp, moved.astype(BF16).astype(F32), False)

    def norm_rows(dp, block, keep):
        inv = lax.rsqrt(jnp.mean(block * block, axis=1, keepdims=True) + 1e-06)
        normed[span(dp), :] = (block * inv * gain_ref[...]).astype(BF16)
        if keep:
            inv_ref[...] = jnp.broadcast_to(inv, inv_ref.shape)

    def forward(dp, count=1, part=0, parts=1):
        def body(cols):
            value, slope = gelu_both(dot_nn(normed[span(dp, count), :], win[:, cols]))
            hidden[span(dp, count), cols] = value.astype(BF16)
            hgrad[span(dp, count), cols] = slope.astype(BF16)

        tiles(body, hidden_units, tile_of(at, TILE if count == 1 else TILE_WIDE), part, parts)

    def flat_grad(gather, dp):
        if narrow:
            grad_flat[span(dp), :] = gather.row_block(dp, width)

    def backward(dp, count=1, part=0, parts=1):
        body = functools.partial(backward_tile, grad_flat, wout_t, hgrad, span(dp, count))
        tiles(body, hidden_units, tile_of(at, TILE if count == 1 else TILE_WIDE), part, parts)

    def partial_out(number, landing):
        sums = ScatterSum(at, outgoing, landing, kept, sum_sems[number])
        for k in sums.order():
            column = pl.multiple_of(sums.chunk(k) * CHUNK, CHUNK)
            sums.give(k, dot_nn(hidden[span(at.dp), :], wout[:, pl.ds(column, CHUNK)]))
        return sums

    partner = at.y * 2 + 1 - at.core
    planes = [(j, lax.rem(at.y + j, at.ys) * 2) for j in range(1, at.ys)]

    def arrive(gather, then):
        for j, plane in planes:
            gather.from_y(j)
        for j, plane in planes:
            gather.from_core(j)
            then(gather, plane)
            then(gather, plane + 1)

    def forward_planes(part):
        for j, plane in planes:
            forward(plane, 2, part, 2)

    def backward_planes(part):
        for j, plane in planes:
            backward(plane, 2, part, 2)

    def finish_forward(sums, perturb, number):
        embedded = tokens_ref[...].astype(F32) + perturb
        out_grad = (embedded + sums.take() - target_ref[...]) * scale
        out_grad_ref[...] = out_grad
        own_grad[number] = pack(out_grad.astype(BF16))

    def turn_weights(part):
        def body(cols):
            wout_t[:, cols] = wout[cols, :].T

        tiles(body, hidden_units, 512, part, 2)

    loads[5].wait()
    turn_weights(0)
    emb.spread()
    turn_weights(1)
    emb.land()
    norm(emb, at.dp, keep=True)
    loads[6].wait()
    forward(at.dp)
    for load in late:
        load.start()
    sums = partial_out(0, landing_1)
    emb.from_core(0)
    norm(emb, partner)
    forward(partner)
    arrive(emb, norm)
    forward_planes(0)
    emb.done()
    finish_forward(sums, adv_init * noise_ref[...], 0)
    grad = Gather(at, own_grad.at[0], grad_all, gather_sems[1])
    forward_planes(1)
    grad.spread()
    turn_in[...] = turned(at, normed, own_cols)
    counts = counting.take()
    scale_ref[...] = jnp.maximum(counts, 1.0) * features
    for step in range(1, at.dp_count):
        ids = count_in[step - 1, 4:5, :]
        onehot_ref[lax.rem(at.dp + at.dp_count - step, at.dp_count)] = members(ids)
    grad.land()

    flat_grad(grad, at.dp)
    backward(at.dp)
    sums = ScatterSum(at, outgoing, landing_2, kept, sum_sems[1])
    row_dot = jnp.zeros((rows, 1), F32)
    for k in sums.order():
        column = pl.multiple_of(sums.chunk(k) * CHUNK, CHUNK)
        value = dot_nt(hgrad[span(at.dp), :], win[pl.ds(column, CHUNK), :])
        sums.give(k, value)
        along = emb_flat[span(at.dp), pl.ds(column, CHUNK)].astype(F32) * gain_ref[:, pl.ds(column, CHUNK)]
        row_dot = row_dot + jnp.sum(value * along, axis=1, keepdims=True)
    table_out[...] = jnp.where(lane == 0.0, row_dot, 0.0).T[:8, :]
    dots = SmallSum(at, "tensor", table_out, table_in, table_sems)
    grad.from_core(0)
    flat_grad(grad, partner)
    backward(partner)
    arrive(grad, flat_grad)
    backward_planes(0)
    scaled = gain_own * sums.take()
    row_dot = jnp.concatenate([dots.take(), jnp.zeros((rows - 8, rows), F32)], axis=0).T[:, 0:1]
    inv = inv_ref[:, :width]
    radial = first_emb().astype(F32) * (inv * inv * inv * (1.0 / features))
    delta = out_grad_ref[...] + inv * scaled - radial * row_dot
    square = jnp.sum(delta * delta, axis=1, keepdims=True)
    square_out[...] = jnp.broadcast_to(
        jnp.sum(onehot_ref[at.dp] * square, axis=0, keepdims=True), (8, rows)
    )
    squares = SmallSum(at, "tensor", square_out, square_in, square_sems)
    out_grad_ref[...] = delta
    own_emb[1] = pack(delta.astype(BF16))
    emb = Gather(at, own_emb.at[1], delta_all, gather_sems[2])
    backward_planes(1)
    emb.spread()
    square_out_dp[...] = squares.take()
    squares = SmallSum(at, "dp", square_out_dp, square_in_dp, square_dp_sems)
    turn_out = turned(at, grad_flat, own_cols)
    for load in late:
        load.wait()

    def moment_in_tile(cols):
        gradient = dot_nn(turn_in[...], hgrad[:, cols])
        mom_in[:, cols] = decay * mom_in[:, cols] + gradient * (1.0 / ASCENTS)

    def moment_out_tile(cols):
        gradient = dot_nn(turn_out, hidden[:, cols]).T
        mom_out[cols, :] = decay * mom_out[cols, :] + gradient * (1.0 / ASCENTS)

    tiles(moment_in_tile, hidden_units, 512)
    grad.done()
    emb.land()
    tiles(moment_out_tile, hidden_units, 512)
    root_mean = jnp.sqrt(squares.take() / scale_ref[...] + 1e-06)
    scale_ref[...] = adv_step / root_mean
    token_scale = jnp.sum(onehot_ref[at.dp] * scale_ref[0:1, :], axis=1, keepdims=True)
    perturb_ref[...] = adv_init * noise_ref[...] + out_grad_ref[...] * token_scale

    norm_moved(emb, at.dp)
    forward(at.dp)
    sums = partial_out(2, landing_3)
    emb.from_core(0)
    norm_moved(emb, partner)
    forward(partner)
    arrive(emb, norm_moved)
    forward_planes(0)
    finish_forward(sums, perturb_ref[...], 1)
    grad = Gather(at, own_grad.at[1], grad_all, gather_sems[3])
    forward_planes(1)
    turn_in[...] = turned(at, normed, own_cols)
    grad.spread()
    grad.land()

    flat_grad(grad, at.dp)
    backward(at.dp)
    grad.from_core(0)
    flat_grad(grad, partner)
    backward(partner)
    arrive(grad, flat_grad)
    emb.done()
    grad.done()


def update_kernel(
    hidden, hgrad, turn_in, mom_in, mom_out, own_in, own_out, wout_t, grad_flat, perturb_ref,
    win_hbm, wout_hbm, min_hbm, mout_hbm, perturb_hbm,
    new_min, new_mout, new_win, new_wout, turn_out, perturb_sem, sems,
):
    at = Place()
    own_cols, hidden_units = mom_in.shape
    pair = perturb_ref.shape[0] * 2
    block_cols = own_out.shape[1]
    tile = tile_of(at, 1024)
    count = hidden_units // tile
    perturb_out = pltpu.make_async_copy(perturb_ref, perturb_hbm, perturb_sem)
    perturb_out.start()
    turn_out[...] = turned(at, grad_flat, own_cols)

    def copies(i):
        cols = pl.ds(pl.multiple_of(i * tile, tile), tile)
        return [
            pltpu.make_async_copy(new_min.at[:, cols], min_hbm.at[:, cols], sems.at[0, i]),
            pltpu.make_async_copy(new_win.at[:, cols], win_hbm.at[:, cols], sems.at[1, i]),
            pltpu.make_async_copy(new_mout.at[cols], mout_hbm.at[cols], sems.at[2, i]),
            pltpu.make_async_copy(new_wout.at[cols], wout_hbm.at[cols], sems.at[3, i]),
        ]

    offset = at.dp * own_cols - at.dp * own_cols // block_cols * block_cols

    @pl.loop(0, count)
    def _(i):
        cols = pl.ds(pl.multiple_of(i * tile, tile), tile)
        gradient = dot_nn(turn_out[...], hidden[:, cols]).T
        moment = decay_rest(mom_out[cols, :], gradient)
        new_mout[cols, :] = moment
        own = own_part(own_out[cols, :].astype(F32), offset, own_cols, 1)
        new_wout[cols, :] = (own - learn_rate * moment).astype(BF16)
        for j in range(1, at.ys):
            start = lax.rem(at.y + j, at.ys) * pair
            backward_tile(grad_flat, wout_t, hgrad, pl.ds(pl.multiple_of(start, pair), pair), cols)
        gradient = dot_nn(turn_in[...], hgrad[:, cols])
        moment = decay_rest(mom_in[:, cols], gradient)
        new_min[:, cols] = moment
        new_win[:, cols] = (own_in[:, cols].astype(F32) - learn_rate * moment).astype(BF16)
        for copy in copies(i):
            copy.start()

    @pl.loop(0, count)
    def _(i):
        for copy in copies(i):
            copy.wait()

    perturb_out.wait()


def decay_rest(moment, gradient):
    return moment + gradient * (1.0 / ASCENTS)


def room(shapes):
    size = 0
    for shape in shapes:
        if shape.memory_space == pltpu.VMEM:
            *outer, last = shape.shape
            lanes = -(-last // LANES) * LANES
            size += functools.reduce(lambda a, b: a * b, outer, lanes) * jnp.dtype(shape.dtype).itemsize
    return size + int(3.25 * 2**20)


def shards(
    tokens, init_noise, segment_ids, target, norm_gain, weight_in, weight_out, moment_in, moment_out
):
    dp_count, tensor_count = lax.axis_size("dp"), lax.axis_size("tensor")
    rows, width = tokens.shape
    features, hidden_units = weight_in.shape
    own_cols = moment_in.shape[0]
    total = rows * dp_count
    narrow = width % LANES != 0
    block_cols = max(own_cols, LANES)
    dma = pltpu.SemaphoreType.DMA
    vmem = pl.BlockSpec(memory_space=pltpu.VMEM)
    anywhere = pl.BlockSpec(memory_space=pltpu.HBM)
    parts = max(1, LANES // width)
    whole = pltpu.VMEM(
        (tensor_count, total // parts, width * parts) if narrow else (total, features), BF16
    )
    landing = pltpu.VMEM((tensor_count - 1, rows, width), BF16)
    small = pltpu.VMEM((8, rows), F32)
    unused = pltpu.VMEM((16, LANES), BF16)
    over_tensor = pltpu.VMEM((tensor_count - 1, 8, rows), F32)
    over_dp = pltpu.VMEM((dp_count - 1, 8, rows), F32)

    def both(count):
        return [dma((count,)), dma((count,))]

    gather = both(gather_copies(dp_count, tensor_count))
    tensor_sems, dp_sems = both(tensor_count - 1), both(dp_count - 1)
    results = (
        pltpu.VMEM((total, hidden_units), BF16),
        pltpu.VMEM((total, hidden_units), BF16),
        pltpu.VMEM((own_cols, total), BF16),
        pltpu.VMEM((own_cols, hidden_units), F32),
        pltpu.VMEM((hidden_units, own_cols), F32),
        pltpu.VMEM((own_cols, hidden_units), BF16),
        pltpu.VMEM((hidden_units, block_cols), BF16),
        pltpu.VMEM((features, hidden_units), BF16),
        pltpu.VMEM((total, features), BF16),
        pltpu.VMEM((rows, width), F32),
    )
    scratch = [
        pltpu.VMEM((rows, width), BF16),
        pltpu.VMEM((rows, width), F32),
        pltpu.VMEM((1, rows), jnp.int32),
        pltpu.VMEM((rows, width), F32),
        pltpu.VMEM((1, features), F32),
        pltpu.VMEM((features, hidden_units), BF16),
        pltpu.VMEM((hidden_units, features), BF16),
        whole,
        pltpu.VMEM((total, features), BF16) if narrow else unused,
        unused if narrow else whole,
        whole if narrow else unused,
        pltpu.VMEM((total, features), BF16),
        pltpu.VMEM((2, rows // parts, width * parts), BF16),
        pltpu.VMEM((2, rows // parts, width * parts), BF16),
        pltpu.VMEM((rows, width), F32),
        pltpu.VMEM((rows, LANES), F32),
        pltpu.VMEM((dp_count, rows, rows), F32),
        small,
        pltpu.VMEM((CHUNK // width, rows, width), F32),
        pltpu.VMEM((tensor_count, rows, width), BF16),
        landing, landing, landing,
        small, over_tensor, small, over_tensor, small, over_dp, small, over_dp,
        dma((7,)), dma((4,)),
        *gather, *gather, *gather, *gather,
        *tensor_sems, *tensor_sems, *tensor_sems,
        *tensor_sems, *tensor_sems, *dp_sems, *dp_sems,
    ]
    kept = pl.pallas_call(
        functools.partial(
            step_kernel, scale=(rows * dp_count) ** (-0.5), features=features
        ),
        name="step",
        out_shape=results,
        in_specs=[anywhere] * 9,
        out_specs=(vmem,) * len(results),
        scratch_shapes=scratch,
        compiler_params=pltpu.CompilerParams(
            collective_id=0, has_side_effects=True, vmem_limit_bytes=room(scratch)
        ),
    )(
        *(
            pltpu.with_memory_space_constraint(array, pltpu.HBM)
            for array in (
                tokens, init_noise, segment_ids.reshape(1, rows), target,
                norm_gain.reshape(1, features), weight_in, weight_out, moment_in, moment_out,
            )
        )
    )
    staged = [
        pltpu.VMEM((own_cols, hidden_units), F32),
        pltpu.VMEM((hidden_units, own_cols), F32),
        pltpu.VMEM((own_cols, hidden_units), BF16),
        pltpu.VMEM((hidden_units, own_cols), BF16),
        pltpu.VMEM((own_cols, total), BF16),
        dma(()),
        dma((4, hidden_units // CHUNK)),
    ]
    return pl.pallas_call(
        update_kernel,
        name="update",
        out_shape=(
            jax.ShapeDtypeStruct((own_cols, hidden_units), BF16),
            jax.ShapeDtypeStruct((hidden_units, own_cols), BF16),
            jax.ShapeDtypeStruct((own_cols, hidden_units), F32),
            jax.ShapeDtypeStruct((hidden_units, own_cols), F32),
            jax.ShapeDtypeStruct((rows, width), F32),
        ),
        in_specs=[vmem] * len(kept),
        out_specs=(anywhere,) * 5,
        scratch_shapes=staged,
        compiler_params=pltpu.CompilerParams(vmem_limit_bytes=max(room(staged), room(scratch))),
    )(*kept)


def solution(mesh):
    placed = (
        P("dp", "tensor"),
        P("dp", "tensor"),
        P("dp"),
        P("dp", "tensor"),
        P(),
        P(None, "tensor"),
        P("tensor", None),
        P("dp", "tensor"),
        P("tensor", "dp"),
    )
    return jax.shard_map(
        shards,
        mesh=mesh,
        in_specs=placed,
        out_specs=(
            P("dp", "tensor"),
            P("tensor", "dp"),
            P("dp", "tensor"),
            P("tensor", "dp"),
            P("dp", "tensor"),
        ),
        check_vma=False,
    )
```

```python
import functools

import jax
import jax.numpy as jnp
from jax import lax
from jax.experimental import pallas as pl
from jax.experimental.pallas import tpu as pltpu
from jax.sharding import PartitionSpec as P

ASCENTS = 2

coeff = 0.7978845608
cubic = 0.044715
adv_init = 0.5
adv_step = 0.5
decay = 0.9
learn_rate = 0.01
LANES = 128
CHUNK = 256
TILE, TILE_WIDE = 2048, 1024
F32, BF16 = jnp.float32, jnp.bfloat16


def gelu_both(values):
    square = values * values
    half = 0.5 + 0.5 * jnp.tanh(values * (coeff + (coeff * cubic) * square))
    hidden = values * half
    slope = half + (hidden * (1.0 - half)) * (2.0 * coeff + (6.0 * coeff * cubic) * square)
    return hidden, slope


def dot_nt(left, right):
    return lax.dot_general(left, right, (((1,), (1,)), ((), ())), preferred_element_type=F32)


def dot_nn(left, right):
    return jnp.dot(left, right, preferred_element_type=F32)


class Place:
    def __init__(self):
        self.dp_count, self.tensor_count = lax.axis_size("dp"), lax.axis_size("tensor")
        self.ys, self.zs = self.dp_count // 2, self.tensor_count // 2
        self.dp, self.tensor = lax.axis_index("dp"), lax.axis_index("tensor")
        self.y, self.core = self.dp // 2, self.dp % 2
        self.z, self.x = self.tensor // 2, self.tensor % 2


def enter(at):
    barrier = pltpu.get_barrier_semaphore()
    for step in range(1, at.tensor_count):
        there = (at.dp, lax.rem(at.tensor + step, at.tensor_count))
        pl.semaphore_signal(barrier, inc=1, device_id=there, device_id_type=pl.DeviceIdType.MESH)
    for step in range(1, at.dp_count):
        there = (lax.rem(at.dp + step, at.dp_count), at.tensor)
        pl.semaphore_signal(barrier, inc=1, device_id=there, device_id_type=pl.DeviceIdType.MESH)


def entered(at):
    pl.semaphore_wait(pltpu.get_barrier_semaphore(), at.tensor_count + at.dp_count - 2)


def send(source, target, sems, number, there, landed=None):
    copy = pltpu.make_async_remote_copy(
        src_ref=source,
        dst_ref=target,
        send_sem=sems[0].at[number],
        recv_sem=sems[1].at[number if landed is None else landed],
        device_id=there,
        device_id_type=pl.DeviceIdType.MESH,
    )
    copy.start()
    return copy


def gather_copies(dp_count, tensor_count):
    ys = dp_count // 2
    return tensor_count + (ys - 1) * tensor_count + ys


def pack(block):
    parts = max(1, LANES // block.shape[1])
    size = block.shape[0] // parts
    return jnp.concatenate([block[i * size:(i + 1) * size] for i in range(parts)], axis=1)


def unpack(block, width):
    return jnp.concatenate(
        [block[:, i:i + width] for i in range(0, block.shape[1], width)], axis=0
    )


class Gather:
    def __init__(self, at, own_ref, whole_ref, sems):
        self.at, self.whole, self.sems = at, whole_ref, sems
        self.rows, self.cols = own_ref.shape
        self.numbers = iter(range(at.zs, gather_copies(at.dp_count, at.tensor_count)))
        self.flat = len(whole_ref.shape) == 2
        self.started = []
        self.other_x = (at.dp, at.z * 2 + 1 - at.x)
        self.partner = (at.y * 2 + 1 - at.core, at.tensor)
        whole_ref[self.place(at.dp, at.tensor)] = own_ref[...]
        own = self.block(at.dp, at.tensor)
        for m in range(at.zs - 1):
            there = (at.dp, self.across(m) * 2 + at.x)
            self.started.append(send(own_ref, own, sems, m, there, landed=at.z))
        self.along_x = [self.start(own_ref, own, self.other_x)]
        self.along_y = {j: [] for j in range(1, at.ys)}
        self.onward(own_ref, own)

    def span(self, dp):
        return pl.ds(pl.multiple_of(dp * self.rows, self.rows), self.rows)

    def place(self, dp, tensor):
        if self.flat:
            return (self.span(dp), pl.ds(pl.multiple_of(tensor * self.cols, self.cols), self.cols))
        return (tensor, self.span(dp))

    def block(self, dp, tensor):
        return self.whole.at[self.place(dp, tensor)]

    def strip(self, dp):
        return self.whole.at[self.span(dp)] if self.flat else self.whole.at[:, self.span(dp)]

    def start(self, source, target, there):
        copy = send(source, target, self.sems, next(self.numbers), there)
        self.started.append(copy)
        return copy

    def across(self, m):
        at = self.at
        upper = at.z // (at.zs // 2)
        last = at.zs - 1 - m
        down = last - (at.z - last + at.zs) // at.zs
        up = m + (m - at.z + at.zs) // at.zs
        return upper * up + (1 - upper) * down

    def nearest(self):
        return [self.across(m) for m in reversed(range(self.at.zs - 1))]

    def onward(self, source, block):
        at = self.at
        for j, copies in self.along_y.items():
            there = (lax.rem(at.y + at.ys - j, at.ys) * 2 + at.core, at.tensor)
            copies.append(self.start(source, block, there))

    def spread(self):
        at = self.at
        for z in self.nearest():
            block = self.block(at.dp, z * 2 + at.x)
            pltpu.make_async_remote_copy(
                src_ref=block,
                dst_ref=block,
                send_sem=self.sems[0].at[0],
                recv_sem=self.sems[1].at[z],
                device_id=self.other_x,
                device_id_type=pl.DeviceIdType.MESH,
            ).wait_recv()
            self.along_x.append(self.start(block, block, self.other_x))
            self.onward(block, block)

    def land(self):
        at = self.at
        for z, copy in zip([at.z] + self.nearest(), self.along_x):
            copy.wait_recv()
            block = self.block(at.dp, z * 2 + 1 - at.x)
            self.onward(block, block)
        strip = self.strip(at.dp)
        self.to_core = {0: self.start(strip, strip, self.partner)}

    def from_y(self, j):
        at = self.at
        for copy in self.along_y[j]:
            copy.wait_recv()
        strip = self.strip(lax.rem(at.y + j, at.ys) * 2 + at.core)
        self.to_core[j] = self.start(strip, strip, self.partner)

    def from_core(self, j):
        self.to_core[j].wait_recv()

    def done(self):
        for copy in self.started:
            copy.wait_send()

    def row_block(self, dp, width):
        if self.flat:
            return self.whole[self.span(dp), :]
        return jnp.concatenate(
            [unpack(self.whole[t, self.span(dp), :], width) for t in range(self.at.tensor_count)],
            axis=1,
        )


class ScatterSum:
    def __init__(self, at, outgoing, landing, kept, sems):
        self.at, self.outgoing, self.landing, self.kept, self.sems = (
            at, outgoing, landing, kept, sems
        )
        self.cols = outgoing.shape[2]
        self.group = CHUNK // self.cols
        self.chunks = at.tensor_count // self.group
        self.inner = at.tensor % self.group
        self.copies = {}

    def order(self):
        half = self.chunks // 2
        return sorted(range(self.chunks), key=lambda k: (k == 0, abs(k - half)))

    def chunk(self, k):
        return lax.rem(self.at.tensor // self.group + k, self.chunks)

    def give(self, k, value):
        first = self.chunk(k) * self.group
        for i in range(self.group):
            part = value[:, i * self.cols:(i + 1) * self.cols]
            self.outgoing[first + i] = part.astype(BF16)
            if k == 0:
                self.kept[i] = part
        for j in range(self.group):
            label = k * self.group + j
            if label:
                there = first + lax.rem(self.inner + j, self.group)
                self.copies[label] = send(
                    self.outgoing.at[there], self.landing.at[label - 1], self.sems, label - 1,
                    (self.at.dp, there),
                )

    def take(self):
        value = self.kept[self.inner]
        for label, copy in self.copies.items():
            copy.wait_recv()
            value = value + self.landing[label - 1].astype(F32)
        for copy in self.copies.values():
            copy.wait_send()
        return value


class SmallSum:
    def __init__(self, at, axis, out, landing, sems):
        count = at.dp_count if axis == "dp" else at.tensor_count
        self.out, self.landing, self.copies = out, landing, []
        for step in range(1, count):
            if axis == "dp":
                there = (lax.rem(at.dp + step, count), at.tensor)
            else:
                there = (at.dp, lax.rem(at.tensor + step, count))
            self.copies.append(send(out, landing.at[step - 1], sems, step - 1, there))

    def take(self):
        value = self.out[...]
        for step, copy in enumerate(self.copies):
            copy.wait_recv()
            value = value + self.landing[step]
        for copy in self.copies:
            copy.wait_send()
        return value


def own_part(value, offset, size, axis):
    parts = [lax.slice_in_dim(value, s, s + size, axis=axis) for s in range(0, value.shape[axis], size)]
    result = parts[0]
    for i, part in enumerate(parts[1:], 1):
        result = jnp.where(offset == i * size, part, result)
    return result


def turned(at, source, own_cols):
    block = max(own_cols, LANES)
    start = at.dp * own_cols // block * block
    value = source[:, pl.ds(pl.multiple_of(start, block), block)].astype(F32).T
    return own_part(value, at.dp * own_cols - start, own_cols, 0).astype(BF16)


def tiles(body, size, tile, part=0, parts=1):
    share = size // tile // parts

    @pl.loop(part * share, (part + 1) * share)
    def _(i):
        body(pl.ds(pl.multiple_of(i * tile, tile), tile))


def tile_of(at, tile):
    return tile if at.ys <= 2 else CHUNK


def backward_tile(grad_flat, wout_t, hgrad, span, cols):
    value = dot_nn(grad_flat[span, :], wout_t[:, cols])
    hgrad[span, cols] = (value * hgrad[span, cols].astype(F32)).astype(BF16)


def step_kernel(
    tokens_hbm, noise_hbm, ids_hbm, target_hbm, gain_hbm, win_hbm, wout_hbm, min_hbm, mout_hbm,
    hidden, hgrad, turn_in, mom_in, mom_out, own_in, own_out, wout_t, grad_flat, perturb_ref,
    tokens_ref, noise_ref, ids_ref, target_ref, gain_ref,
    win, wout, emb_all, emb_kept, delta_whole, grad_3d, normed, own_emb, own_grad, out_grad_ref, inv_ref,
    onehot_ref, scale_ref, kept, outgoing, landing_1, landing_2, landing_3,
    table_out, table_in, square_out, square_in, square_out_dp, square_in_dp, count_out, count_in,
    load_sems, late_sems, *sems, scale, features,
):
    at = Place()
    rows, width = tokens_ref.shape
    hidden_units = win.shape[1]
    own_cols = mom_in.shape[0]
    pairs = [(sems[2 * i], sems[2 * i + 1]) for i in range(len(sems) // 2)]
    gather_sems, sum_sems = pairs[:4], pairs[4:7]
    table_sems, square_sems, square_dp_sems, count_sems = pairs[7:11]
    narrow = len(emb_all.shape) == 3
    grad_all = grad_3d if narrow else grad_flat
    emb_flat = emb_kept if narrow else emb_all
    delta_all = emb_all if narrow else delta_whole

    small = [(tokens_hbm, tokens_ref), (noise_hbm, noise_ref)]
    small += [(ids_hbm, ids_ref), (gain_hbm, gain_ref), (target_hbm, target_ref)]
    loads = [
        pltpu.make_async_copy(source, target, load_sems.at[i])
        for i, (source, target) in enumerate(small + [(wout_hbm, wout), (win_hbm, win)])
    ]
    for load in loads:
        load.start()
    block_cols = own_out.shape[1]
    first_col = at.dp * own_cols // block_cols * block_cols
    late = [
        pltpu.make_async_copy(
            win_hbm.at[pl.ds(pl.multiple_of(at.dp * own_cols, own_cols), own_cols)], own_in,
            late_sems.at[0],
        ),
        pltpu.make_async_copy(
            wout_hbm.at[:, pl.ds(pl.multiple_of(first_col, block_cols), block_cols)], own_out,
            late_sems.at[1],
        ),
        pltpu.make_async_copy(min_hbm, mom_in, late_sems.at[2]),
        pltpu.make_async_copy(mout_hbm, mom_out, late_sems.at[3]),
    ]
    enter(at)
    for load in loads[:5]:
        load.wait()
    def first_emb():
        return (tokens_ref[...].astype(F32) + adv_init * noise_ref[...]).astype(BF16)

    own_emb[0] = pack(first_emb())
    entered(at)
    emb = Gather(at, own_emb.at[0], emb_all, gather_sems[0])

    lane = lax.broadcasted_iota(jnp.int32, (rows, rows), 1).astype(F32)

    def members(ids):
        return (jnp.broadcast_to(ids, (rows, rows)).T == lane).astype(BF16)

    onehot_ref[at.dp] = members(ids_ref[...].astype(F32))
    count_out[0:4, :] = jnp.broadcast_to(
        jnp.sum(onehot_ref[at.dp].astype(F32), axis=0, keepdims=True), (4, rows)
    )
    count_out[4:8, :] = jnp.broadcast_to(ids_ref[...].astype(F32), (4, rows))
    counting = SmallSum(at, "dp", count_out, count_in, count_sems)
    group = max(width, LANES)
    first = at.tensor * width // group * group
    gain_own = own_part(
        gain_ref[:, pl.ds(pl.multiple_of(first, group), group)], at.tensor * width - first, width, 1
    )

    def span(dp, count=1):
        return pl.ds(pl.multiple_of(dp * rows, count * rows), count * rows)

    def norm(gather, dp, keep=False):
        block = gather.row_block(dp, width)
        if narrow:
            emb_flat[span(dp), :] = block
        norm_rows(dp, block.astype(F32), keep)

    def norm_moved(gather, dp):
        step = jnp.sum(onehot_ref[dp].astype(F32) * scale_ref[0:1, :], axis=1, keepdims=True)
        moved = emb_flat[span(dp), :].astype(F32) + step * gather.row_block(dp, width).astype(F32)
        norm_rows(dp, moved.astype(BF16).astype(F32), False)

    def norm_rows(dp, block, keep):
        inv = lax.rsqrt(jnp.mean(block * block, axis=1, keepdims=True) + 1e-06)
        normed[span(dp), :] = (block * inv * gain_ref[...]).astype(BF16)
        if keep:
            inv_ref[...] = jnp.broadcast_to(inv, inv_ref.shape)

    def forward(dp, count=1, part=0, parts=1):
        def body(cols):
            value, slope = gelu_both(dot_nn(normed[span(dp, count), :], win[:, cols]))
            hidden[span(dp, count), cols] = value.astype(BF16)
            hgrad[span(dp, count), cols] = slope.astype(BF16)

        tiles(body, hidden_units, tile_of(at, TILE if count == 1 else TILE_WIDE), part, parts)

    def flat_grad(gather, dp):
        if narrow:
            grad_flat[span(dp), :] = gather.row_block(dp, width)

    def backward(dp, count=1, part=0, parts=1):
        body = functools.partial(backward_tile, grad_flat, wout_t, hgrad, span(dp, count))
        tiles(body, hidden_units, tile_of(at, TILE if count == 1 else TILE_WIDE), part, parts)

    def partial_out(number, landing):
        sums = ScatterSum(at, outgoing, landing, kept, sum_sems[number])
        for k in sums.order():
            column = pl.multiple_of(sums.chunk(k) * CHUNK, CHUNK)
            sums.give(k, dot_nn(hidden[span(at.dp), :], wout[:, pl.ds(column, CHUNK)]))
        return sums

    partner = at.y * 2 + 1 - at.core
    planes = [(j, lax.rem(at.y + j, at.ys) * 2) for j in range(1, at.ys)]

    def arrive(gather, then):
        for j, plane in planes:
            gather.from_y(j)
        for j, plane in planes:
            gather.from_core(j)
            then(gather, plane)
            then(gather, plane + 1)

    def forward_planes(part):
        for j, plane in planes:
            forward(plane, 2, part, 4)

    def backward_planes(part):
        for j, plane in planes:
            backward(plane, 2, part, 2)

    def finish_forward(sums, perturb, number):
        embedded = tokens_ref[...].astype(F32) + perturb
        out_grad = (embedded + sums.take() - target_ref[...]) * scale
        out_grad_ref[...] = out_grad
        own_grad[0] = pack(out_grad.astype(BF16))

    def turn_weights(part):
        def body(cols):
            wout_t[:, cols] = wout[cols, :].T

        tiles(body, hidden_units, 512, part, 2)

    emb.spread()
    loads[5].wait()
    turn_weights(0)
    emb.land()
    norm(emb, at.dp, keep=True)
    loads[6].wait()
    forward(at.dp)
    for load in late:
        load.start()
    sums = partial_out(0, landing_1)
    emb.from_core(0)
    norm(emb, partner)
    forward(partner)
    arrive(emb, norm)
    forward_planes(0)
    emb.done()
    finish_forward(sums, adv_init * noise_ref[...], 0)
    grad = Gather(at, own_grad.at[0], grad_all, gather_sems[1])
    forward_planes(1)
    grad.spread()
    forward_planes(2)
    forward_planes(3)
    turn_weights(1)
    turn_in[...] = turned(at, normed, own_cols)
    counts = counting.take()
    scale_ref[...] = jnp.maximum(counts, 1.0) * features
    for step in range(1, at.dp_count):
        ids = count_in[step - 1, 4:5, :]
        onehot_ref[lax.rem(at.dp + at.dp_count - step, at.dp_count)] = members(ids)
    grad.land()

    flat_grad(grad, at.dp)
    backward(at.dp)
    sums = ScatterSum(at, outgoing, landing_2, kept, sum_sems[1])
    row_dot = jnp.zeros((rows, 1), F32)
    for k in sums.order():
        column = pl.multiple_of(sums.chunk(k) * CHUNK, CHUNK)
        value = dot_nt(hgrad[span(at.dp), :], win[pl.ds(column, CHUNK), :])
        sums.give(k, value)
        along = emb_flat[span(at.dp), pl.ds(column, CHUNK)].astype(F32) * gain_ref[:, pl.ds(column, CHUNK)]
        row_dot = row_dot + jnp.sum(value * along, axis=1, keepdims=True)
    table_out[...] = jnp.where(lane == 0.0, row_dot, 0.0).T[:8, :]
    dots = SmallSum(at, "tensor", table_out, table_in, table_sems)
    grad.from_core(0)
    flat_grad(grad, partner)
    backward(partner)
    arrive(grad, flat_grad)
    backward_planes(0)
    scaled = gain_own * sums.take()
    row_dot = jnp.concatenate([dots.take(), jnp.zeros((rows - 8, rows), F32)], axis=0).T[:, 0:1]
    inv = inv_ref[:, :width]
    radial = first_emb().astype(F32) * (inv * inv * inv * (1.0 / features))
    delta = out_grad_ref[...] + inv * scaled - radial * row_dot
    square = jnp.sum(delta * delta, axis=1, keepdims=True)
    square_out[...] = jnp.broadcast_to(
        jnp.sum(onehot_ref[at.dp].astype(F32) * square, axis=0, keepdims=True), (8, rows)
    )
    squares = SmallSum(at, "tensor", square_out, square_in, square_sems)
    out_grad_ref[...] = delta
    own_emb[0] = pack(delta.astype(BF16))
    emb = Gather(at, own_emb.at[0], delta_all, gather_sems[2])
    backward_planes(1)
    emb.spread()
    square_out_dp[...] = squares.take()
    squares = SmallSum(at, "dp", square_out_dp, square_in_dp, square_dp_sems)
    turn_out = turned(at, grad_flat, own_cols)
    for load in late:
        load.wait()

    def moment_in_tile(cols):
        gradient = dot_nn(turn_in[...], hgrad[:, cols])
        mom_in[:, cols] = decay * mom_in[:, cols] + gradient * (1.0 / ASCENTS)

    def moment_out_tile(cols):
        gradient = dot_nn(turn_out, hidden[:, cols]).T
        mom_out[cols, :] = decay * mom_out[cols, :] + gradient * (1.0 / ASCENTS)

    tiles(moment_in_tile, hidden_units, tile_of(at, 1024))
    grad.done()
    emb.land()
    tiles(moment_out_tile, hidden_units, tile_of(at, 1024))
    root_mean = jnp.sqrt(squares.take() / scale_ref[...] + 1e-06)
    scale_ref[...] = adv_step / root_mean
    token_scale = jnp.sum(onehot_ref[at.dp].astype(F32) * scale_ref[0:1, :], axis=1, keepdims=True)
    perturb_ref[...] = adv_init * noise_ref[...] + out_grad_ref[...] * token_scale

    norm_moved(emb, at.dp)
    forward(at.dp)
    sums = partial_out(2, landing_3)
    emb.from_core(0)
    norm_moved(emb, partner)
    forward(partner)
    arrive(emb, norm_moved)
    forward_planes(0)
    finish_forward(sums, perturb_ref[...], 1)
    grad = Gather(at, own_grad.at[0], grad_all, gather_sems[3])
    forward_planes(1)
    grad.spread()
    forward_planes(2)
    forward_planes(3)
    turn_in[...] = turned(at, normed, own_cols)
    grad.land()

    flat_grad(grad, at.dp)
    backward(at.dp)
    grad.from_core(0)
    flat_grad(grad, partner)
    backward(partner)
    arrive(grad, flat_grad)
    emb.done()
    grad.done()


def update_kernel(
    hidden, hgrad, turn_in, mom_in, mom_out, own_in, own_out, wout_t, grad_flat, perturb_ref,
    win_hbm, wout_hbm, min_hbm, mout_hbm, perturb_hbm,
    new_min, new_mout, new_win, new_wout, turn_out, perturb_sem, sems,
):
    at = Place()
    own_cols, hidden_units = mom_in.shape
    pair = perturb_ref.shape[0] * 2
    block_cols = own_out.shape[1]
    tile = tile_of(at, 1024)
    count = hidden_units // tile
    perturb_out = pltpu.make_async_copy(perturb_ref, perturb_hbm, perturb_sem)
    perturb_out.start()
    turn_out[...] = turned(at, grad_flat, own_cols)

    def copies(i):
        cols = pl.ds(pl.multiple_of(i * tile, tile), tile)
        return [
            pltpu.make_async_copy(new_min.at[:, cols], min_hbm.at[:, cols], sems.at[0, i]),
            pltpu.make_async_copy(new_win.at[:, cols], win_hbm.at[:, cols], sems.at[1, i]),
            pltpu.make_async_copy(new_mout.at[cols], mout_hbm.at[cols], sems.at[2, i]),
            pltpu.make_async_copy(new_wout.at[cols], wout_hbm.at[cols], sems.at[3, i]),
        ]

    offset = at.dp * own_cols - at.dp * own_cols // block_cols * block_cols

    @pl.loop(0, count)
    def _(i):
        cols = pl.ds(pl.multiple_of(i * tile, tile), tile)
        gradient = dot_nn(turn_out[...], hidden[:, cols]).T
        moment = decay_rest(mom_out[cols, :], gradient)
        new_mout[cols, :] = moment
        own = own_part(own_out[cols, :].astype(F32), offset, own_cols, 1)
        new_wout[cols, :] = (own - learn_rate * moment).astype(BF16)
        for j in range(1, at.ys):
            start = lax.rem(at.y + j, at.ys) * pair
            backward_tile(grad_flat, wout_t, hgrad, pl.ds(pl.multiple_of(start, pair), pair), cols)
        gradient = dot_nn(turn_in[...], hgrad[:, cols])
        moment = decay_rest(mom_in[:, cols], gradient)
        new_min[:, cols] = moment
        new_win[:, cols] = (own_in[:, cols].astype(F32) - learn_rate * moment).astype(BF16)
        for copy in copies(i):
            copy.start()

    @pl.loop(0, count)
    def _(i):
        for copy in copies(i):
            copy.wait()

    perturb_out.wait()


def decay_rest(moment, gradient):
    return moment + gradient * (1.0 / ASCENTS)


def room(shapes):
    size = 0
    for shape in shapes:
        if shape.memory_space == pltpu.VMEM:
            *outer, last = shape.shape
            lanes = -(-last // LANES) * LANES
            size += functools.reduce(lambda a, b: a * b, outer, lanes) * jnp.dtype(shape.dtype).itemsize
    return size + int(3.9 * 2**20)


def shards(
    tokens, init_noise, segment_ids, target, norm_gain, weight_in, weight_out, moment_in, moment_out
):
    dp_count, tensor_count = lax.axis_size("dp"), lax.axis_size("tensor")
    rows, width = tokens.shape
    features, hidden_units = weight_in.shape
    own_cols = moment_in.shape[0]
    total = rows * dp_count
    narrow = width % LANES != 0
    block_cols = max(own_cols, LANES)
    dma = pltpu.SemaphoreType.DMA
    vmem = pl.BlockSpec(memory_space=pltpu.VMEM)
    anywhere = pl.BlockSpec(memory_space=pltpu.HBM)
    parts = max(1, LANES // width)
    whole = pltpu.VMEM(
        (tensor_count, total // parts, width * parts) if narrow else (total, features), BF16
    )
    landing = pltpu.VMEM((tensor_count - 1, rows, width), BF16)
    small = pltpu.VMEM((8, rows), F32)
    unused = pltpu.VMEM((16, LANES), BF16)
    over_tensor = pltpu.VMEM((tensor_count - 1, 8, rows), F32)
    over_dp = pltpu.VMEM((dp_count - 1, 8, rows), F32)

    def both(count):
        return [dma((count,)), dma((count,))]

    gather = both(gather_copies(dp_count, tensor_count))
    tensor_sems, dp_sems = both(tensor_count - 1), both(dp_count - 1)
    results = (
        pltpu.VMEM((total, hidden_units), BF16),
        pltpu.VMEM((total, hidden_units), BF16),
        pltpu.VMEM((own_cols, total), BF16),
        pltpu.VMEM((own_cols, hidden_units), F32),
        pltpu.VMEM((hidden_units, own_cols), F32),
        pltpu.VMEM((own_cols, hidden_units), BF16),
        pltpu.VMEM((hidden_units, block_cols), BF16),
        pltpu.VMEM((features, hidden_units), BF16),
        pltpu.VMEM((total, features), BF16),
        pltpu.VMEM((rows, width), F32),
    )
    scratch = [
        pltpu.VMEM((rows, width), BF16),
        pltpu.VMEM((rows, width), F32),
        pltpu.VMEM((1, rows), jnp.int32),
        pltpu.VMEM((rows, width), F32),
        pltpu.VMEM((1, features), F32),
        pltpu.VMEM((features, hidden_units), BF16),
        pltpu.VMEM((hidden_units, features), BF16),
        whole,
        pltpu.VMEM((total, features), BF16) if narrow else unused,
        unused if narrow else whole,
        whole if narrow else unused,
        pltpu.VMEM((total, features), BF16),
        pltpu.VMEM((1, rows // parts, width * parts), BF16),
        pltpu.VMEM((1, rows // parts, width * parts), BF16),
        pltpu.VMEM((rows, width), F32),
        pltpu.VMEM((rows, LANES), F32),
        pltpu.VMEM((dp_count, rows, rows), BF16),
        small,
        pltpu.VMEM((CHUNK // width, rows, width), F32),
        pltpu.VMEM((tensor_count, rows, width), BF16),
        landing, landing, landing,
        small, over_tensor, small, over_tensor, small, over_dp, small, over_dp,
        dma((7,)), dma((4,)),
        *gather, *gather, *gather, *gather,
        *tensor_sems, *tensor_sems, *tensor_sems,
        *tensor_sems, *tensor_sems, *dp_sems, *dp_sems,
    ]
    kept = pl.pallas_call(
        functools.partial(
            step_kernel, scale=(rows * dp_count) ** (-0.5), features=features
        ),
        name="step",
        out_shape=results,
        in_specs=[anywhere] * 9,
        out_specs=(vmem,) * len(results),
        scratch_shapes=scratch,
        compiler_params=pltpu.CompilerParams(
            collective_id=0, has_side_effects=True, vmem_limit_bytes=room(scratch)
        ),
    )(
        *(
            pltpu.with_memory_space_constraint(array, pltpu.HBM)
            for array in (
                tokens, init_noise, segment_ids.reshape(1, rows), target,
                norm_gain.reshape(1, features), weight_in, weight_out, moment_in, moment_out,
            )
        )
    )
    staged = [
        pltpu.VMEM((own_cols, hidden_units), F32),
        pltpu.VMEM((hidden_units, own_cols), F32),
        pltpu.VMEM((own_cols, hidden_units), BF16),
        pltpu.VMEM((hidden_units, own_cols), BF16),
        pltpu.VMEM((own_cols, total), BF16),
        dma(()),
        dma((4, hidden_units // CHUNK)),
    ]
    return pl.pallas_call(
        update_kernel,
        name="update",
        out_shape=(
            jax.ShapeDtypeStruct((own_cols, hidden_units), BF16),
            jax.ShapeDtypeStruct((hidden_units, own_cols), BF16),
            jax.ShapeDtypeStruct((own_cols, hidden_units), F32),
            jax.ShapeDtypeStruct((hidden_units, own_cols), F32),
            jax.ShapeDtypeStruct((rows, width), F32),
        ),
        in_specs=[vmem] * len(kept),
        out_specs=(anywhere,) * 5,
        scratch_shapes=staged,
        compiler_params=pltpu.CompilerParams(vmem_limit_bytes=max(room(staged), room(scratch))),
    )(*kept)


def solution(mesh):
    placed = (
        P("dp", "tensor"),
        P("dp", "tensor"),
        P("dp"),
        P("dp", "tensor"),
        P(),
        P(None, "tensor"),
        P("tensor", None),
        P("dp", "tensor"),
        P("tensor", "dp"),
    )
    return jax.shard_map(
        shards,
        mesh=mesh,
        in_specs=placed,
        out_specs=(
            P("dp", "tensor"),
            P("tensor", "dp"),
            P("dp", "tensor"),
            P("tensor", "dp"),
            P("dp", "tensor"),
        ),
        check_vma=False,
    )
```

```python
import functools

import jax
import jax.numpy as jnp
from jax import lax
from jax.experimental import pallas as pl
from jax.experimental.pallas import tpu as pltpu
from jax.sharding import PartitionSpec as P

ASCENTS = 2

coeff = 0.7978845608
cubic = 0.044715
adv_init = 0.5
adv_step = 0.5
decay = 0.9
learn_rate = 0.01
LANES = 128
CHUNK = 256
TILE, TILE_WIDE = 2048, 1024
F32, BF16 = jnp.float32, jnp.bfloat16


def gelu_both(values):
    square = values * values
    half = 0.5 + 0.5 * jnp.tanh(values * (coeff + (coeff * cubic) * square))
    hidden = values * half
    slope = half + (hidden * (1.0 - half)) * (2.0 * coeff + (6.0 * coeff * cubic) * square)
    return hidden, slope


def dot_nt(left, right):
    return lax.dot_general(left, right, (((1,), (1,)), ((), ())), preferred_element_type=F32)


def dot_nn(left, right):
    return jnp.dot(left, right, preferred_element_type=F32)


class Place:
    def __init__(self):
        self.dp_count, self.tensor_count = lax.axis_size("dp"), lax.axis_size("tensor")
        self.ys, self.zs = self.dp_count // 2, self.tensor_count // 2
        self.dp, self.tensor = lax.axis_index("dp"), lax.axis_index("tensor")
        self.y, self.core = self.dp // 2, self.dp % 2
        self.z, self.x = self.tensor // 2, self.tensor % 2


def enter(at):
    barrier = pltpu.get_barrier_semaphore()
    for step in range(1, at.tensor_count):
        there = (at.dp, lax.rem(at.tensor + step, at.tensor_count))
        pl.semaphore_signal(barrier, inc=1, device_id=there, device_id_type=pl.DeviceIdType.MESH)
    for step in range(1, at.dp_count):
        there = (lax.rem(at.dp + step, at.dp_count), at.tensor)
        pl.semaphore_signal(barrier, inc=1, device_id=there, device_id_type=pl.DeviceIdType.MESH)


def entered(at):
    pl.semaphore_wait(pltpu.get_barrier_semaphore(), at.tensor_count + at.dp_count - 2)


def send(source, target, sems, number, there, landed=None):
    copy = pltpu.make_async_remote_copy(
        src_ref=source,
        dst_ref=target,
        send_sem=sems[0].at[number],
        recv_sem=sems[1].at[number if landed is None else landed],
        device_id=there,
        device_id_type=pl.DeviceIdType.MESH,
    )
    copy.start()
    return copy


def gather_copies(dp_count, tensor_count):
    ys = dp_count // 2
    return tensor_count + (ys - 1) * tensor_count + ys


def pack(block):
    parts = max(1, LANES // block.shape[1])
    size = block.shape[0] // parts
    return jnp.concatenate([block[i * size:(i + 1) * size] for i in range(parts)], axis=1)


def unpack(block, width):
    return jnp.concatenate(
        [block[:, i:i + width] for i in range(0, block.shape[1], width)], axis=0
    )


class Gather:
    def __init__(self, at, own_ref, whole_ref, sems):
        self.at, self.whole, self.sems = at, whole_ref, sems
        self.rows, self.cols = own_ref.shape
        self.numbers = iter(range(at.zs, gather_copies(at.dp_count, at.tensor_count)))
        self.flat = len(whole_ref.shape) == 2
        self.started = []
        self.other_x = (at.dp, at.z * 2 + 1 - at.x)
        self.partner = (at.y * 2 + 1 - at.core, at.tensor)
        whole_ref[self.place(at.dp, at.tensor)] = own_ref[...]
        own = self.block(at.dp, at.tensor)
        for m in range(at.zs - 1):
            there = (at.dp, self.across(m) * 2 + at.x)
            self.started.append(send(own_ref, own, sems, m, there, landed=at.z))
        self.along_x = [self.start(own_ref, own, self.other_x)]
        self.along_y = {j: [] for j in range(1, at.ys)}
        self.onward(own_ref, own)

    def span(self, dp):
        return pl.ds(pl.multiple_of(dp * self.rows, self.rows), self.rows)

    def place(self, dp, tensor):
        if self.flat:
            return (self.span(dp), pl.ds(pl.multiple_of(tensor * self.cols, self.cols), self.cols))
        return (tensor, self.span(dp))

    def block(self, dp, tensor):
        return self.whole.at[self.place(dp, tensor)]

    def strip(self, dp):
        return self.whole.at[self.span(dp)] if self.flat else self.whole.at[:, self.span(dp)]

    def start(self, source, target, there):
        copy = send(source, target, self.sems, next(self.numbers), there)
        self.started.append(copy)
        return copy

    def across(self, m):
        at = self.at
        upper = at.z // (at.zs // 2)
        last = at.zs - 1 - m
        down = last - (at.z - last + at.zs) // at.zs
        up = m + (m - at.z + at.zs) // at.zs
        return upper * up + (1 - upper) * down

    def nearest(self):
        return [self.across(m) for m in reversed(range(self.at.zs - 1))]

    def onward(self, source, block):
        at = self.at
        for j, copies in self.along_y.items():
            there = (lax.rem(at.y + at.ys - j, at.ys) * 2 + at.core, at.tensor)
            copies.append(self.start(source, block, there))

    def spread(self):
        at = self.at
        for z in self.nearest():
            block = self.block(at.dp, z * 2 + at.x)
            pltpu.make_async_remote_copy(
                src_ref=block,
                dst_ref=block,
                send_sem=self.sems[0].at[0],
                recv_sem=self.sems[1].at[z],
                device_id=self.other_x,
                device_id_type=pl.DeviceIdType.MESH,
            ).wait_recv()
            self.along_x.append(self.start(block, block, self.other_x))
            self.onward(block, block)

    def land(self):
        at = self.at
        for z, copy in zip([at.z] + self.nearest(), self.along_x):
            copy.wait_recv()
            block = self.block(at.dp, z * 2 + 1 - at.x)
            self.onward(block, block)
        strip = self.strip(at.dp)
        self.to_core = {0: self.start(strip, strip, self.partner)}

    def from_y(self, j):
        at = self.at
        for copy in self.along_y[j]:
            copy.wait_recv()
        strip = self.strip(lax.rem(at.y + j, at.ys) * 2 + at.core)
        self.to_core[j] = self.start(strip, strip, self.partner)

    def from_core(self, j):
        self.to_core[j].wait_recv()

    def done(self):
        for copy in self.started:
            copy.wait_send()

    def row_block(self, dp, width):
        if self.flat:
            return self.whole[self.span(dp), :]
        return jnp.concatenate(
            [unpack(self.whole[t, self.span(dp), :], width) for t in range(self.at.tensor_count)],
            axis=1,
        )


class ScatterSum:
    def __init__(self, at, outgoing, landing, kept, sems):
        self.at, self.outgoing, self.landing, self.kept, self.sems = (
            at, outgoing, landing, kept, sems
        )
        self.cols = outgoing.shape[2]
        self.group = CHUNK // self.cols
        self.chunks = at.tensor_count // self.group
        self.inner = at.tensor % self.group
        self.copies = {}

    def order(self):
        half = self.chunks // 2
        return sorted(range(self.chunks), key=lambda k: (k == 0, abs(k - half)))

    def chunk(self, k):
        return lax.rem(self.at.tensor // self.group + k, self.chunks)

    def give(self, k, value):
        first = self.chunk(k) * self.group
        for i in range(self.group):
            part = value[:, i * self.cols:(i + 1) * self.cols]
            self.outgoing[first + i] = part.astype(BF16)
            if k == 0:
                self.kept[i] = part
        for j in range(self.group):
            label = k * self.group + j
            if label:
                there = first + lax.rem(self.inner + j, self.group)
                self.copies[label] = send(
                    self.outgoing.at[there], self.landing.at[label - 1], self.sems, label - 1,
                    (self.at.dp, there),
                )

    def take(self):
        value = self.kept[self.inner]
        for label, copy in self.copies.items():
            copy.wait_recv()
            value = value + self.landing[label - 1].astype(F32)
        for copy in self.copies.values():
            copy.wait_send()
        return value


class SmallSum:
    def __init__(self, at, axis, out, landing, sems):
        count = at.dp_count if axis == "dp" else at.tensor_count
        self.out, self.landing, self.copies = out, landing, []
        for step in range(1, count):
            if axis == "dp":
                there = (lax.rem(at.dp + step, count), at.tensor)
            else:
                there = (at.dp, lax.rem(at.tensor + step, count))
            self.copies.append(send(out, landing.at[step - 1], sems, step - 1, there))

    def take(self):
        value = self.out[...]
        for step, copy in enumerate(self.copies):
            copy.wait_recv()
            value = value + self.landing[step]
        for copy in self.copies:
            copy.wait_send()
        return value


def own_part(value, offset, size, axis):
    parts = [lax.slice_in_dim(value, s, s + size, axis=axis) for s in range(0, value.shape[axis], size)]
    result = parts[0]
    for i, part in enumerate(parts[1:], 1):
        result = jnp.where(offset == i * size, part, result)
    return result


def turned(at, source, own_cols):
    block = max(own_cols, LANES)
    start = at.dp * own_cols // block * block
    value = source[:, pl.ds(pl.multiple_of(start, block), block)].astype(F32).T
    return own_part(value, at.dp * own_cols - start, own_cols, 0).astype(BF16)


def tiles(body, size, tile, part=0, parts=1):
    share = size // tile // parts

    @pl.loop(part * share, (part + 1) * share)
    def _(i):
        body(pl.ds(pl.multiple_of(i * tile, tile), tile))


def tile_of(at, tile):
    return tile if at.ys <= 2 else CHUNK


def backward_tile(grad_flat, wout_t, hgrad, span, cols):
    value = dot_nn(grad_flat[span, :], wout_t[:, cols])
    hgrad[span, cols] = (value * hgrad[span, cols].astype(F32)).astype(BF16)


def step_kernel(
    tokens_hbm, noise_hbm, ids_hbm, target_hbm, gain_hbm, win_hbm, wout_hbm, min_hbm, mout_hbm,
    hidden, hgrad, turn_in, mom_in, mom_out, own_in, own_out, wout_t, grad_flat, perturb_ref,
    tokens_ref, noise_ref, ids_ref, target_ref, gain_ref,
    win, wout, emb_all, emb_kept, delta_whole, grad_3d, normed, own_emb, own_grad, out_grad_ref, inv_ref,
    onehot_ref, scale_ref, kept, outgoing, landing_1, landing_2, landing_3,
    table_out, table_in, square_out, square_in, square_out_dp, square_in_dp, count_out, count_in,
    load_sems, late_sems, *sems, scale, features,
):
    at = Place()
    rows, width = tokens_ref.shape
    hidden_units = win.shape[1]
    own_cols = mom_in.shape[0]
    pairs = [(sems[2 * i], sems[2 * i + 1]) for i in range(len(sems) // 2)]
    gather_sems, sum_sems = pairs[:4], pairs[4:7]
    table_sems, square_sems, square_dp_sems, count_sems = pairs[7:11]
    narrow = len(emb_all.shape) == 3
    grad_all = grad_3d if narrow else grad_flat
    emb_flat = emb_kept if narrow else emb_all
    delta_all = emb_all if narrow else delta_whole

    small = [(tokens_hbm, tokens_ref), (noise_hbm, noise_ref)]
    small += [(ids_hbm, ids_ref), (gain_hbm, gain_ref), (target_hbm, target_ref)]
    loads = [
        pltpu.make_async_copy(source, target, load_sems.at[i])
        for i, (source, target) in enumerate(small + [(wout_hbm, wout), (win_hbm, win)])
    ]
    for load in loads:
        load.start()
    block_cols = own_out.shape[1]
    first_col = at.dp * own_cols // block_cols * block_cols
    late = [
        pltpu.make_async_copy(
            win_hbm.at[pl.ds(pl.multiple_of(at.dp * own_cols, own_cols), own_cols)], own_in,
            late_sems.at[0],
        ),
        pltpu.make_async_copy(
            wout_hbm.at[:, pl.ds(pl.multiple_of(first_col, block_cols), block_cols)], own_out,
            late_sems.at[1],
        ),
        pltpu.make_async_copy(min_hbm, mom_in, late_sems.at[2]),
        pltpu.make_async_copy(mout_hbm, mom_out, late_sems.at[3]),
    ]
    enter(at)
    for load in loads[:5]:
        load.wait()
    def first_emb():
        return (tokens_ref[...].astype(F32) + adv_init * noise_ref[...]).astype(BF16)

    own_emb[0] = pack(first_emb())
    entered(at)
    emb = Gather(at, own_emb.at[0], emb_all, gather_sems[0])

    lane = lax.broadcasted_iota(jnp.int32, (rows, rows), 1).astype(F32)

    def members(ids):
        return (jnp.broadcast_to(ids, (rows, rows)).T == lane).astype(BF16)

    onehot_ref[at.dp] = members(ids_ref[...].astype(F32))
    count_out[0:4, :] = jnp.broadcast_to(
        jnp.sum(onehot_ref[at.dp].astype(F32), axis=0, keepdims=True), (4, rows)
    )
    count_out[4:8, :] = jnp.broadcast_to(ids_ref[...].astype(F32), (4, rows))
    counting = SmallSum(at, "dp", count_out, count_in, count_sems)
    group = max(width, LANES)
    first = at.tensor * width // group * group
    gain_own = own_part(
        gain_ref[:, pl.ds(pl.multiple_of(first, group), group)], at.tensor * width - first, width, 1
    )

    def span(dp, count=1):
        return pl.ds(pl.multiple_of(dp * rows, count * rows), count * rows)

    def norm(gather, dp, keep=False):
        block = gather.row_block(dp, width)
        if narrow:
            emb_flat[span(dp), :] = block
        norm_rows(dp, block.astype(F32), keep)

    def norm_moved(gather, dp):
        step = jnp.sum(onehot_ref[dp].astype(F32) * scale_ref[0:1, :], axis=1, keepdims=True)
        moved = emb_flat[span(dp), :].astype(F32) + step * gather.row_block(dp, width).astype(F32)
        norm_rows(dp, moved.astype(BF16).astype(F32), False)

    def norm_rows(dp, block, keep):
        inv = lax.rsqrt(jnp.mean(block * block, axis=1, keepdims=True) + 1e-06)
        normed[span(dp), :] = (block * inv * gain_ref[...]).astype(BF16)
        if keep:
            inv_ref[...] = jnp.broadcast_to(inv, inv_ref.shape)

    def forward(dp, count=1, part=0, parts=1):
        def body(cols):
            value, slope = gelu_both(dot_nn(normed[span(dp, count), :], win[:, cols]))
            hidden[span(dp, count), cols] = value.astype(BF16)
            hgrad[span(dp, count), cols] = slope.astype(BF16)

        tiles(body, hidden_units, tile_of(at, TILE if count == 1 else TILE_WIDE), part, parts)

    def flat_grad(gather, dp):
        if narrow:
            grad_flat[span(dp), :] = gather.row_block(dp, width)

    def backward(dp, count=1, part=0, parts=1):
        body = functools.partial(backward_tile, grad_flat, wout_t, hgrad, span(dp, count))
        tiles(body, hidden_units, tile_of(at, TILE if count == 1 else TILE_WIDE), part, parts)

    def partial_out(number, landing):
        sums = ScatterSum(at, outgoing, landing, kept, sum_sems[number])
        for k in sums.order():
            column = pl.multiple_of(sums.chunk(k) * CHUNK, CHUNK)
            sums.give(k, dot_nn(hidden[span(at.dp), :], wout[:, pl.ds(column, CHUNK)]))
        return sums

    partner = at.y * 2 + 1 - at.core
    planes = [(j, lax.rem(at.y + j, at.ys) * 2) for j in range(1, at.ys)]

    def arrive(gather, then):
        for j, plane in planes:
            gather.from_y(j)
        for j, plane in planes:
            gather.from_core(j)
            then(gather, plane)
            then(gather, plane + 1)

    def forward_planes(part):
        for j, plane in planes:
            forward(plane, 2, part, 4)

    def backward_planes(part):
        for j, plane in planes:
            backward(plane, 2, part, 2)

    def finish_forward(sums, perturb, number):
        embedded = tokens_ref[...].astype(F32) + perturb
        out_grad = (embedded + sums.take() - target_ref[...]) * scale
        out_grad_ref[...] = out_grad
        own_grad[0] = pack(out_grad.astype(BF16))

    def turn_weights(part):
        def body(cols):
            wout_t[:, cols] = wout[cols, :].T

        tiles(body, hidden_units, 512, part, 2)

    emb.spread()
    loads[5].wait()
    turn_weights(0)
    emb.land()
    norm(emb, at.dp, keep=True)
    loads[6].wait()
    forward(at.dp)
    for load in late:
        load.start()
    sums = partial_out(0, landing_1)
    emb.from_core(0)
    norm(emb, partner)
    forward(partner)
    arrive(emb, norm)
    emb.done()
    finish_forward(sums, adv_init * noise_ref[...], 0)
    grad = Gather(at, own_grad.at[0], grad_all, gather_sems[1])
    forward_planes(1)
    grad.spread()
    forward_planes(0)
    forward_planes(2)
    forward_planes(3)
    turn_weights(1)
    turn_in[...] = turned(at, normed, own_cols)
    counts = counting.take()
    scale_ref[...] = jnp.maximum(counts, 1.0) * features
    for step in range(1, at.dp_count):
        ids = count_in[step - 1, 4:5, :]
        onehot_ref[lax.rem(at.dp + at.dp_count - step, at.dp_count)] = members(ids)
    grad.land()

    flat_grad(grad, at.dp)
    backward(at.dp)
    sums = ScatterSum(at, outgoing, landing_2, kept, sum_sems[1])
    row_dot = jnp.zeros((rows, 1), F32)
    for k in sums.order():
        column = pl.multiple_of(sums.chunk(k) * CHUNK, CHUNK)
        value = dot_nt(hgrad[span(at.dp), :], win[pl.ds(column, CHUNK), :])
        sums.give(k, value)
        along = emb_flat[span(at.dp), pl.ds(column, CHUNK)].astype(F32) * gain_ref[:, pl.ds(column, CHUNK)]
        row_dot = row_dot + jnp.sum(value * along, axis=1, keepdims=True)
    table_out[...] = jnp.where(lane == 0.0, row_dot, 0.0).T[:8, :]
    dots = SmallSum(at, "tensor", table_out, table_in, table_sems)
    grad.from_core(0)
    flat_grad(grad, partner)
    backward(partner)
    arrive(grad, flat_grad)
    backward_planes(0)
    scaled = gain_own * sums.take()
    row_dot = jnp.concatenate([dots.take(), jnp.zeros((rows - 8, rows), F32)], axis=0).T[:, 0:1]
    inv = inv_ref[:, :width]
    radial = first_emb().astype(F32) * (inv * inv * inv * (1.0 / features))
    delta = out_grad_ref[...] + inv * scaled - radial * row_dot
    square = jnp.sum(delta * delta, axis=1, keepdims=True)
    square_out[...] = jnp.broadcast_to(
        jnp.sum(onehot_ref[at.dp].astype(F32) * square, axis=0, keepdims=True), (8, rows)
    )
    squares = SmallSum(at, "tensor", square_out, square_in, square_sems)
    out_grad_ref[...] = delta
    own_emb[0] = pack(delta.astype(BF16))
    emb = Gather(at, own_emb.at[0], delta_all, gather_sems[2])
    backward_planes(1)
    emb.spread()
    square_out_dp[...] = squares.take()
    squares = SmallSum(at, "dp", square_out_dp, square_in_dp, square_dp_sems)
    turn_out = turned(at, grad_flat, own_cols)
    for load in late:
        load.wait()

    def moment_in_tile(cols):
        gradient = dot_nn(turn_in[...], hgrad[:, cols])
        mom_in[:, cols] = decay * mom_in[:, cols] + gradient * (1.0 / ASCENTS)

    def moment_out_tile(cols):
        gradient = dot_nn(turn_out, hidden[:, cols]).T
        mom_out[cols, :] = decay * mom_out[cols, :] + gradient * (1.0 / ASCENTS)

    tiles(moment_in_tile, hidden_units, tile_of(at, 1024))
    grad.done()
    emb.land()
    tiles(moment_out_tile, hidden_units, tile_of(at, 1024))
    root_mean = jnp.sqrt(squares.take() / scale_ref[...] + 1e-06)
    scale_ref[...] = adv_step / root_mean
    token_scale = jnp.sum(onehot_ref[at.dp].astype(F32) * scale_ref[0:1, :], axis=1, keepdims=True)
    perturb_ref[...] = adv_init * noise_ref[...] + out_grad_ref[...] * token_scale

    norm_moved(emb, at.dp)
    forward(at.dp)
    sums = partial_out(2, landing_3)
    emb.from_core(0)
    norm_moved(emb, partner)
    forward(partner)
    arrive(emb, norm_moved)
    finish_forward(sums, perturb_ref[...], 1)
    grad = Gather(at, own_grad.at[0], grad_all, gather_sems[3])
    forward_planes(1)
    grad.spread()
    forward_planes(0)
    forward_planes(2)
    forward_planes(3)
    turn_in[...] = turned(at, normed, own_cols)
    grad.land()

    flat_grad(grad, at.dp)
    backward(at.dp)
    grad.from_core(0)
    flat_grad(grad, partner)
    backward(partner)
    arrive(grad, flat_grad)
    emb.done()
    grad.done()


def update_kernel(
    hidden, hgrad, turn_in, mom_in, mom_out, own_in, own_out, wout_t, grad_flat, perturb_ref,
    win_hbm, wout_hbm, min_hbm, mout_hbm, perturb_hbm,
    new_min, new_mout, new_win, new_wout, turn_out, perturb_sem, sems,
):
    at = Place()
    own_cols, hidden_units = mom_in.shape
    pair = perturb_ref.shape[0] * 2
    block_cols = own_out.shape[1]
    tile = tile_of(at, 1024)
    count = hidden_units // tile
    perturb_out = pltpu.make_async_copy(perturb_ref, perturb_hbm, perturb_sem)
    perturb_out.start()
    turn_out[...] = turned(at, grad_flat, own_cols)

    def copies(i):
        cols = pl.ds(pl.multiple_of(i * tile, tile), tile)
        return [
            pltpu.make_async_copy(new_min.at[:, cols], min_hbm.at[:, cols], sems.at[0, i]),
            pltpu.make_async_copy(new_win.at[:, cols], win_hbm.at[:, cols], sems.at[1, i]),
            pltpu.make_async_copy(new_mout.at[cols], mout_hbm.at[cols], sems.at[2, i]),
            pltpu.make_async_copy(new_wout.at[cols], wout_hbm.at[cols], sems.at[3, i]),
        ]

    offset = at.dp * own_cols - at.dp * own_cols // block_cols * block_cols

    @pl.loop(0, count)
    def _(i):
        cols = pl.ds(pl.multiple_of(i * tile, tile), tile)
        gradient = dot_nn(turn_out[...], hidden[:, cols]).T
        moment = decay_rest(mom_out[cols, :], gradient)
        new_mout[cols, :] = moment
        own = own_part(own_out[cols, :].astype(F32), offset, own_cols, 1)
        new_wout[cols, :] = (own - learn_rate * moment).astype(BF16)
        for j in range(1, at.ys):
            start = lax.rem(at.y + j, at.ys) * pair
            backward_tile(grad_flat, wout_t, hgrad, pl.ds(pl.multiple_of(start, pair), pair), cols)
        gradient = dot_nn(turn_in[...], hgrad[:, cols])
        moment = decay_rest(mom_in[:, cols], gradient)
        new_min[:, cols] = moment
        new_win[:, cols] = (own_in[:, cols].astype(F32) - learn_rate * moment).astype(BF16)
        for copy in copies(i):
            copy.start()

    @pl.loop(0, count)
    def _(i):
        for copy in copies(i):
            copy.wait()

    perturb_out.wait()


def decay_rest(moment, gradient):
    return moment + gradient * (1.0 / ASCENTS)


def room(shapes):
    size = 0
    for shape in shapes:
        if shape.memory_space == pltpu.VMEM:
            *outer, last = shape.shape
            lanes = -(-last // LANES) * LANES
            size += functools.reduce(lambda a, b: a * b, outer, lanes) * jnp.dtype(shape.dtype).itemsize
    return size + int(3.9 * 2**20)


def shards(
    tokens, init_noise, segment_ids, target, norm_gain, weight_in, weight_out, moment_in, moment_out
):
    dp_count, tensor_count = lax.axis_size("dp"), lax.axis_size("tensor")
    rows, width = tokens.shape
    features, hidden_units = weight_in.shape
    own_cols = moment_in.shape[0]
    total = rows * dp_count
    narrow = width % LANES != 0
    block_cols = max(own_cols, LANES)
    dma = pltpu.SemaphoreType.DMA
    vmem = pl.BlockSpec(memory_space=pltpu.VMEM)
    anywhere = pl.BlockSpec(memory_space=pltpu.HBM)
    parts = max(1, LANES // width)
    whole = pltpu.VMEM(
        (tensor_count, total // parts, width * parts) if narrow else (total, features), BF16
    )
    landing = pltpu.VMEM((tensor_count - 1, rows, width), BF16)
    small = pltpu.VMEM((8, rows), F32)
    unused = pltpu.VMEM((16, LANES), BF16)
    over_tensor = pltpu.VMEM((tensor_count - 1, 8, rows), F32)
    over_dp = pltpu.VMEM((dp_count - 1, 8, rows), F32)

    def both(count):
        return [dma((count,)), dma((count,))]

    gather = both(gather_copies(dp_count, tensor_count))
    tensor_sems, dp_sems = both(tensor_count - 1), both(dp_count - 1)
    results = (
        pltpu.VMEM((total, hidden_units), BF16),
        pltpu.VMEM((total, hidden_units), BF16),
        pltpu.VMEM((own_cols, total), BF16),
        pltpu.VMEM((own_cols, hidden_units), F32),
        pltpu.VMEM((hidden_units, own_cols), F32),
        pltpu.VMEM((own_cols, hidden_units), BF16),
        pltpu.VMEM((hidden_units, block_cols), BF16),
        pltpu.VMEM((features, hidden_units), BF16),
        pltpu.VMEM((total, features), BF16),
        pltpu.VMEM((rows, width), F32),
    )
    scratch = [
        pltpu.VMEM((rows, width), BF16),
        pltpu.VMEM((rows, width), F32),
        pltpu.VMEM((1, rows), jnp.int32),
        pltpu.VMEM((rows, width), F32),
        pltpu.VMEM((1, features), F32),
        pltpu.VMEM((features, hidden_units), BF16),
        pltpu.VMEM((hidden_units, features), BF16),
        whole,
        pltpu.VMEM((total, features), BF16) if narrow else unused,
        unused if narrow else whole,
        whole if narrow else unused,
        pltpu.VMEM((total, features), BF16),
        pltpu.VMEM((1, rows // parts, width * parts), BF16),
        pltpu.VMEM((1, rows // parts, width * parts), BF16),
        pltpu.VMEM((rows, width), F32),
        pltpu.VMEM((rows, LANES), F32),
        pltpu.VMEM((dp_count, rows, rows), BF16),
        small,
        pltpu.VMEM((CHUNK // width, rows, width), F32),
        pltpu.VMEM((tensor_count, rows, width), BF16),
        landing, landing, landing,
        small, over_tensor, small, over_tensor, small, over_dp, small, over_dp,
        dma((7,)), dma((4,)),
        *gather, *gather, *gather, *gather,
        *tensor_sems, *tensor_sems, *tensor_sems,
        *tensor_sems, *tensor_sems, *dp_sems, *dp_sems,
    ]
    kept = pl.pallas_call(
        functools.partial(
            step_kernel, scale=(rows * dp_count) ** (-0.5), features=features
        ),
        name="step",
        out_shape=results,
        in_specs=[anywhere] * 9,
        out_specs=(vmem,) * len(results),
        scratch_shapes=scratch,
        compiler_params=pltpu.CompilerParams(
            collective_id=0, has_side_effects=True, vmem_limit_bytes=room(scratch)
        ),
    )(
        *(
            pltpu.with_memory_space_constraint(array, pltpu.HBM)
            for array in (
                tokens, init_noise, segment_ids.reshape(1, rows), target,
                norm_gain.reshape(1, features), weight_in, weight_out, moment_in, moment_out,
            )
        )
    )
    staged = [
        pltpu.VMEM((own_cols, hidden_units), F32),
        pltpu.VMEM((hidden_units, own_cols), F32),
        pltpu.VMEM((own_cols, hidden_units), BF16),
        pltpu.VMEM((hidden_units, own_cols), BF16),
        pltpu.VMEM((own_cols, total), BF16),
        dma(()),
        dma((4, hidden_units // CHUNK)),
    ]
    return pl.pallas_call(
        update_kernel,
        name="update",
        out_shape=(
            jax.ShapeDtypeStruct((own_cols, hidden_units), BF16),
            jax.ShapeDtypeStruct((hidden_units, own_cols), BF16),
            jax.ShapeDtypeStruct((own_cols, hidden_units), F32),
            jax.ShapeDtypeStruct((hidden_units, own_cols), F32),
            jax.ShapeDtypeStruct((rows, width), F32),
        ),
        in_specs=[vmem] * len(kept),
        out_specs=(anywhere,) * 5,
        scratch_shapes=staged,
        compiler_params=pltpu.CompilerParams(vmem_limit_bytes=max(room(staged), room(scratch))),
    )(*kept)


def solution(mesh):
    placed = (
        P("dp", "tensor"),
        P("dp", "tensor"),
        P("dp"),
        P("dp", "tensor"),
        P(),
        P(None, "tensor"),
        P("tensor", None),
        P("dp", "tensor"),
        P("tensor", "dp"),
    )
    return jax.shard_map(
        shards,
        mesh=mesh,
        in_specs=placed,
        out_specs=(
            P("dp", "tensor"),
            P("tensor", "dp"),
            P("dp", "tensor"),
            P("tensor", "dp"),
            P("dp", "tensor"),
        ),
        check_vma=False,
    )
```
